256 devices in a mesh: shard: 32 (over z_lo, y, core), model: 8 (over z_hi, x).
Axes of the slice: x: 4, y: 4, z: 8 (z_hi: 2, z_lo: 4; z = z_hi * 4 + z_lo), core: 2. Of those that a mesh axis runs over, the one named last changes fastest.
Arguments:
- gradients: float32 [256, 128, 4096], P(None, 'shard', 'model'), may hold values from -6 to 6
- momentum: float32 [256, 128, 4096], P(None, 'shard', 'model'), may hold values from -6 to 6
- weights: float32 [256, 128, 4096], P(None, 'shard', 'model'), may hold values from -0.1875 to 0.1875
Outputs:
- new_weights: float32 [256, 128, 4096], P(None, 'shard', 'model')
- new_momentum: float32 [256, 128, 4096], P(None, 'shard', 'model')
The draws below stay inside these ranges and needn't reach their ends.
All inputs are finite; a program needn't handle non-finite values.
Results may differ from the reference program's by a relative error of at most 0.00012.
Values sent between devices are 32-bit elements; how exact they have to be, the bound alone decides.
A program may use at most 64 MiB of HBM per device.

```python
import jax
import jax.numpy as jnp
from jax import lax

SIDE = 128
WIDE = 4096
MATS = 256
ITERS = 4


def steps_of(key, dims, pieces, smallest, top_value):
    level = 1.0
    for dim, parts in pieces:
        heights = jax.random.uniform(jax.random.fold_in(jax.random.fold_in(key, 6), dim), (parts,), jnp.float32, smallest / len(pieces), top_value / len(pieces))
        level = level * jnp.repeat(jnp.exp(heights), dims[dim] // parts).reshape((-1,) + (1,) * (len(dims) - 1 - dim))
    return level


def gaussian(stream_key, dims, width, bound, split=(), kind=jnp.bfloat16):
    result = jax.random.normal(stream_key, dims, jnp.float32) * width
    if len(split) > 0:
        result = steps_of(stream_key, dims, split, -0.22, 0.18) * result
    return jnp.clip(result, min=-bound, max=bound).astype(kind)


def setup_inputs(seed: int = 0) -> dict:
    keys = jax.random.split(jax.random.key(seed), 4)
    return {
        "gradients": gaussian(keys[0], (MATS, SIDE, WIDE), 1.0, 6.0, ((1, 32), (2, 8)), jnp.float32),
        "momentum": gaussian(keys[1], (MATS, SIDE, WIDE), 1.0, 6.0, ((1, 32), (2, 8)), jnp.float32),
        "weights": gaussian(keys[2], (MATS, SIDE, WIDE), 0.03, 0.1875, ((1, 32), (2, 8)), jnp.float32),
    }


hold_rate = 0.9
learn_rate = 0.8

def reference(gradients, momentum, weights):
    new_momentum = hold_rate * momentum + gradients
    direction = hold_rate * new_momentum + gradients

    def orthogonal_one(stack):
        iterate = stack[None]
        iterate = iterate * lax.rsqrt(lax.optimization_barrier(jnp.sum(iterate * iterate, axis=(1, 2), keepdims=True)) + 1e-06)
        for step in range(ITERS):
            gram = jnp.einsum('mik,mjk->mij', iterate, iterate, precision=lax.Precision.HIGHEST)
            mixed = -4.775 * gram + 2.0315 * jnp.einsum('mij,mjk->mik', gram, gram, precision=lax.Precision.HIGHEST)
            iterate = 3.4445 * iterate + jnp.einsum('mij,mjk->mik', mixed, iterate, precision=lax.Precision.HIGHEST)
        return iterate[0]
    iterate = lax.map(orthogonal_one, direction)
    new_weights = weights - learn_rate * iterate
    return (new_weights, new_momentum)
```

```python
import functools

import jax
import jax.numpy as jnp
from jax import lax
from jax.experimental import pallas as pl
from jax.experimental.pallas import tpu as pltpu
from jax.sharding import PartitionSpec as P

MESH = pl.DeviceIdType.MESH
F32 = jnp.float32
ITERS = 4
ROUNDS = 2
PER = 4
hold_rate = 0.9
learn_rate = 0.8
HI = lax.Precision.HIGHEST


def dot(a, b):
    return lax.dot_general(a, b, (((1,), (0,)), ((), ())), precision=HI, preferred_element_type=F32)


def dot_t(a, b):
    return lax.dot_general(a, b, (((1,), (1,)), ((), ())), precision=HI, preferred_element_type=F32)


def merge_halves(a, b):
    low = lax.broadcasted_iota(jnp.int32, a.shape, 1) < 4
    return (
        jnp.where(low, a, pltpu.roll(b, 4, 1)),
        jnp.where(low, pltpu.roll(a, 4, 1), b),
    )


def kernel(
    g_hbm, m_hbm, back,
    gbuf, mbuf, D, R, X, G, GX, S, Z, QR, Y,
    gsem, msem, p1s, p1r, xs, xr, zs, zr, qs, qr, p2s, p2r, own1, own2,
):
    s, m = lax.axis_index("shard"), lax.axis_index("model")
    zl, yy, core = s // 8, (s // 2) % 4, s % 2
    zh, x = m // 4, m % 4
    side = zl // 2

    def group_of(d):
        z = d // 8
        return (zh * (3 - z) + (1 - zh) * z) * 8 + d % 8

    mine = group_of(s)
    partner = ((3 - zl) * 8 + s % 8, (1 - zh) * 4 + x)

    def dest(k):
        c, a, b = k // 16, (k % 16) // 4, k % 4
        z = side * a + (1 - side) * (3 - a)
        return z * 8 + ((yy + 2 + b) % 4) * 2 + c

    barrier = pltpu.get_barrier_semaphore()

    @pl.loop(1, 32)
    def _(k):
        pl.semaphore_signal(barrier, inc=1, device_id=((s + k) % 32, m), device_id_type=MESH)

    for k in range(1, 4):
        pl.semaphore_signal(barrier, inc=1, device_id=(s, zh * 4 + (x + k) % 4), device_id_type=MESH)
    pl.semaphore_signal(barrier, inc=1, device_id=partner, device_id_type=MESH)

    pieces, size = 4, 1024
    loads = []
    for i in range(pieces):
        part = pl.ds(i * size, size)
        loads.append((
            pltpu.make_async_copy(g_hbm.at[part], gbuf.at[part], gsem.at[i]),
            pltpu.make_async_copy(m_hbm.at[part], mbuf.at[part], msem.at[i]),
        ))
        loads[-1][0].start()
        loads[-1][1].start()
    for i in range(pieces):
        loads[i][0].wait()
        loads[i][1].wait()

        @pl.loop(0, size // 128)
        def _(b):
            rows = pl.ds(pl.multiple_of(i * size + b * 128, 128), 128)
            g = gbuf[rows, :]
            D[rows, :] = hold_rate * (hold_rate * mbuf[rows, :] + g) + g

    pl.semaphore_wait(barrier, 35)

    def p1_copy(r, d):
        t = group_of(d)
        return pltpu.make_async_remote_copy(
            src_ref=D.at[pl.ds(pl.multiple_of(t * 128 + r * 64, 64), 64), :],
            dst_ref=R.at[r, s // 2, s % 2],
            send_sem=p1s.at[r, d],
            recv_sem=p1r.at[r, s],
            device_id=(d, m),
            device_id_type=MESH,
        )

    def p1_from(r, q):
        return pltpu.make_async_remote_copy(
            src_ref=D.at[pl.ds(0, 64), :],
            dst_ref=R.at[r, q // 2, q % 2],
            send_sem=p1s.at[r, q],
            recv_sem=p1r.at[r, q],
            device_id=(q, m),
            device_id_type=MESH,
        )

    def p1_own(r):
        return pltpu.make_async_copy(
            D.at[pl.ds(pl.multiple_of(mine * 128 + r * 64, 64), 64), :], R.at[r, s // 2, s % 2], own1.at[r]
        )

    for r in range(ROUNDS):
        @pl.loop(0, 32)
        def _(k):
            d = dest(k)

            @pl.when(d != s)
            def _():
                p1_copy(r, d).start()

        p1_own(r).start()

    eye = (
        lax.broadcasted_iota(jnp.int32, (128, 128), 0) == lax.broadcasted_iota(jnp.int32, (128, 128), 1)
    ).astype(F32)

    def x_copy(r, to, slot):
        return pltpu.make_async_remote_copy(
            src_ref=G.at[r, to],
            dst_ref=GX.at[r, slot],
            send_sem=xs.at[r, to],
            recv_sem=xr.at[r, slot],
            device_id=(s, zh * 4 + to),
            device_id_type=MESH,
        )

    def q_copy(r, to, slot):
        return pltpu.make_async_remote_copy(
            src_ref=QR.at[r, slot],
            dst_ref=QR.at[r, slot],
            send_sem=qs.at[r, to],
            recv_sem=qr.at[r, slot],
            device_id=(s, zh * 4 + to),
            device_id_type=MESH,
        )

    def z_copy(r):
        return pltpu.make_async_remote_copy(
            src_ref=S.at[r], dst_ref=Z.at[r], send_sem=zs.at[r], recv_sem=zr.at[r],
            device_id=partner, device_id_type=MESH,
        )

    def p2_rows(t, r):
        return back.at[pl.ds(pl.multiple_of(t * 128 + r * 64, 64), 64), :]

    def p2_copy(r, d):
        return pltpu.make_async_remote_copy(
            src_ref=Y.at[r, d // 2, d % 2], dst_ref=p2_rows(mine, r), send_sem=p2s.at[r, d], recv_sem=p2r.at[r, s],
            device_id=(d, m), device_id_type=MESH,
        )

    def p2_from(r, q):
        return pltpu.make_async_remote_copy(
            src_ref=Y.at[r, q // 2, q % 2], dst_ref=p2_rows(group_of(q), r), send_sem=p2s.at[r, q],
            recv_sem=p2r.at[r, q], device_id=(q, m), device_id_type=MESH,
        )

    def p2_own(r):
        return pltpu.make_async_copy(Y.at[r, s // 2, s % 2], p2_rows(mine, r), own2.at[r])

    for r in range(ROUNDS):
        @pl.loop(1, 32)
        def _(k):
            p1_from(r, (s + k) % 32).wait_recv()

        p1_own(r).wait()

        @pl.loop(0, PER)
        def _(j):
            for h in range(2):
                rows = pl.ds(pl.multiple_of(j * 16 + h * 8, 8), 8)
                low, high = merge_halves(R[r, :, 0, rows, :], R[r, :, 1, rows, :])
                X[j, :, 256 * h : 256 * h + 128] = low.reshape(128, 128)
                X[j, :, 256 * h + 128 : 256 * h + 256] = high.reshape(128, 128)
            G[r, j] = dot_t(X[j], X[j])

        for k in range(1, 4):
            x_copy(r, (x + k) % 4, x).start()
        total = G[r, x]
        for k in range(1, 4):
            q = (x + k) % 4
            x_copy(r, q, q).wait_recv()
            total = total + GX[r, q]
        S[r] = total
        z_copy(r).start()
        z_copy(r).wait_recv()
        gram = S[r] + Z[r]
        scale = lax.rsqrt(jnp.sum(jnp.sum(gram * eye, axis=1, keepdims=True), axis=0, keepdims=True) + 1e-06)
        gram = gram * (scale * scale)
        factor = None
        for step in range(ITERS):
            mixed = 3.4445 * eye + (-4.775 * gram + 2.0315 * dot(gram, gram))
            factor = mixed if factor is None else dot(mixed, factor)
            if step < ITERS - 1:
                gram = dot(dot(mixed, gram), mixed)
        QR[r, x] = factor * scale
        for k in range(1, 4):
            q_copy(r, (x + k) % 4, x).start()
        for k in range(1, 4):
            q = (x + k) % 4
            q_copy(r, q, q).wait_recv()

        @pl.loop(0, PER)
        def _(j):
            for h in range(2):
                wide = dot(QR[r, j], X[j, :, 256 * h : 256 * h + 256])
                rows = pl.ds(pl.multiple_of(j * 16 + h * 8, 8), 8)
                even, odd = merge_halves(wide[:, :128].reshape(16, 8, 128), wide[:, 128:].reshape(16, 8, 128))
                Y[r, :, 0, rows, :] = even
                Y[r, :, 1, rows, :] = odd

        @pl.loop(0, 32)
        def _(k):
            d = dest(k)

            @pl.when(d != s)
            def _():
                p2_copy(r, d).start()

        p2_own(r).start()

    for r in range(ROUNDS):
        @pl.loop(1, 32)
        def _(k):
            q = (s + k) % 32
            p2_from(r, q).wait_recv()
            p1_copy(r, q).wait_send()
            p2_copy(r, q).wait_send()

        p2_own(r).wait()
        z_copy(r).wait_send()
        for k in range(1, 4):
            x_copy(r, (x + k) % 4, x).wait_send()
            q_copy(r, (x + k) % 4, x).wait_send()


def exchange(g, m):
    dma = pltpu.SemaphoreType.DMA
    return pl.pallas_call(
        kernel,
        out_shape=jax.ShapeDtypeStruct((4096, 128), F32),
        in_specs=[pl.BlockSpec(memory_space=pl.ANY)] * 2,
        out_specs=pl.BlockSpec(memory_space=pl.ANY),
        scratch_shapes=[
            pltpu.VMEM((4096, 128), F32),
            pltpu.VMEM((4096, 128), F32),
            pltpu.VMEM((4096, 128), F32),
            pltpu.VMEM((ROUNDS, 16, 2, 64, 128), F32),
            pltpu.VMEM((PER, 128, 512), F32),
            pltpu.VMEM((ROUNDS, PER, 128, 128), F32),
            pltpu.VMEM((ROUNDS, 4, 128, 128), F32),
            pltpu.VMEM((ROUNDS, 128, 128), F32),
            pltpu.VMEM((ROUNDS, 128, 128), F32),
            pltpu.VMEM((ROUNDS, 4, 128, 128), F32),
            pltpu.VMEM((ROUNDS, 16, 2, 64, 128), F32),
            dma((4,)), dma((4,)),
            dma((ROUNDS, 32)), dma((ROUNDS, 32)),
            dma((ROUNDS, 4)), dma((ROUNDS, 4)),
            dma((ROUNDS,)), dma((ROUNDS,)),
            dma((ROUNDS, 4)), dma((ROUNDS, 4)),
            dma((ROUNDS, 32)), dma((ROUNDS, 32)),
            dma((ROUNDS,)), dma((ROUNDS,)),
        ],
        compiler_params=pltpu.CompilerParams(
            collective_id=0, has_side_effects=True, vmem_limit_bytes=40 * 1024 * 1024
        ),
        name="exchange",
    )(g, m)


def flat(a):
    return a.reshape(256, 4, 4, 128).transpose(0, 2, 1, 3).reshape(4096, 128)


def unflat(a):
    return a.reshape(256, 4, 4, 128).transpose(0, 2, 1, 3).reshape(256, 4, 512)


def local(gradients, momentum, weights):
    g, m, w = flat(gradients), flat(momentum), flat(weights)
    back = exchange(g, m)
    new_momentum = hold_rate * m + g
    new_weights = w - learn_rate * back
    return (unflat(new_weights), unflat(new_momentum))


def solution(mesh):
    placed = P(None, "shard", "model")
    return jax.shard_map(
        local, mesh=mesh, in_specs=(placed,) * 3, out_specs=(placed, placed), check_vma=False
    )
```

```python
import functools

import jax
import jax.numpy as jnp
from jax import lax
from jax.experimental import pallas as pl
from jax.experimental.pallas import tpu as pltpu
from jax.sharding import PartitionSpec as P

MESH = pl.DeviceIdType.MESH
F32 = jnp.float32
ITERS = 4
ROUNDS = 2
PER = 4
hold_rate = 0.9
learn_rate = 0.8
HI = lax.Precision.HIGHEST


def dot(a, b):
    return lax.dot_general(a, b, (((1,), (0,)), ((), ())), precision=HI, preferred_element_type=F32)


def dot_t(a, b):
    return lax.dot_general(a, b, (((1,), (1,)), ((), ())), precision=HI, preferred_element_type=F32)


def merge_halves(a, b):
    low = lax.broadcasted_iota(jnp.int32, a.shape, 1) < 4
    return (
        jnp.where(low, a, pltpu.roll(b, 4, 1)),
        jnp.where(low, pltpu.roll(a, 4, 1), b),
    )


def kernel(
    g_hbm, m_hbm, back, moved,
    gbuf, mbuf, D, R, X, G, GX, S, Z, QR, Y,
    gsem, msem, p1s, p1r, xs, xr, zs, zr, qs, qr, p2s, p2r, own1, own2,
):
    s, m = lax.axis_index("shard"), lax.axis_index("model")
    zl, yy, core = s // 8, (s // 2) % 4, s % 2
    zh, x = m // 4, m % 4
    side = zl // 2

    def group_of(d):
        z = d // 8
        return (zh * (3 - z) + (1 - zh) * z) * 8 + d % 8

    mine = group_of(s)
    partner = ((3 - zl) * 8 + s % 8, (1 - zh) * 4 + x)

    def dest(k):
        c, a, b = k // 16, (k % 16) // 4, k % 4
        z = side * a + (1 - side) * (3 - a)
        return z * 8 + ((yy + 2 + b) % 4) * 2 + 1 - c

    pieces, size = 4, 1024
    loads = []
    for i in range(pieces):
        part = pl.ds(i * size, size)
        loads.append((
            pltpu.make_async_copy(g_hbm.at[part], gbuf.at[part], gsem.at[i]),
            pltpu.make_async_copy(m_hbm.at[part], mbuf.at[part], msem.at[i]),
        ))
        loads[-1][0].start()
        loads[-1][1].start()

    barrier = pltpu.get_barrier_semaphore()

    @pl.loop(1, 32)
    def _(k):
        pl.semaphore_signal(barrier, inc=1, device_id=((s + k) % 32, m), device_id_type=MESH)

    for k in range(1, 4):
        pl.semaphore_signal(barrier, inc=1, device_id=(s, zh * 4 + (x + k) % 4), device_id_type=MESH)
    pl.semaphore_signal(barrier, inc=1, device_id=partner, device_id_type=MESH)

    for i in range(pieces):
        loads[i][0].wait()
        loads[i][1].wait()

        @pl.loop(0, size // 128)
        def _(b):
            rows = pl.ds(pl.multiple_of(i * size + b * 128, 128), 128)
            g = gbuf[rows, :]
            D[rows, :] = hold_rate * (hold_rate * mbuf[rows, :] + g) + g

    pl.semaphore_wait(barrier, 35)

    def p1_copy(r, d):
        t = group_of(d)
        return pltpu.make_async_remote_copy(
            src_ref=D.at[pl.ds(pl.multiple_of(t * 128 + r * 64, 64), 64), :],
            dst_ref=R.at[r, s // 2, s % 2],
            send_sem=p1s.at[r, d],
            recv_sem=p1r.at[r, s],
            device_id=(d, m),
            device_id_type=MESH,
        )

    def p1_from(r, q):
        return pltpu.make_async_remote_copy(
            src_ref=D.at[pl.ds(0, 64), :],
            dst_ref=R.at[r, q // 2, q % 2],
            send_sem=p1s.at[r, q],
            recv_sem=p1r.at[r, q],
            device_id=(q, m),
            device_id_type=MESH,
        )

    def p1_own(r):
        return pltpu.make_async_copy(
            D.at[pl.ds(pl.multiple_of(mine * 128 + r * 64, 64), 64), :], R.at[r, s // 2, s % 2], own1.at[r]
        )

    for r in range(ROUNDS):
        @pl.loop(0, 32)
        def _(k):
            d = dest(k)

            @pl.when(d != s)
            def _():
                p1_copy(r, d).start()

        p1_own(r).start()

    eye = (
        lax.broadcasted_iota(jnp.int32, (128, 128), 0) == lax.broadcasted_iota(jnp.int32, (128, 128), 1)
    ).astype(F32)

    def x_copy(r, to, slot):
        return pltpu.make_async_remote_copy(
            src_ref=G.at[r, to],
            dst_ref=GX.at[r, slot],
            send_sem=xs.at[r, to],
            recv_sem=xr.at[r, slot],
            device_id=(s, zh * 4 + to),
            device_id_type=MESH,
        )

    def q_copy(r, to, slot):
        return pltpu.make_async_remote_copy(
            src_ref=QR.at[r, slot],
            dst_ref=QR.at[r, slot],
            send_sem=qs.at[r, to],
            recv_sem=qr.at[r, slot],
            device_id=(s, zh * 4 + to),
            device_id_type=MESH,
        )

    def z_copy(r):
        return pltpu.make_async_remote_copy(
            src_ref=S.at[r], dst_ref=Z.at[r], send_sem=zs.at[r], recv_sem=zr.at[r],
            device_id=partner, device_id_type=MESH,
        )

    def p2_rows(t, r):
        return back.at[pl.ds(pl.multiple_of(t * 128 + r * 64, 64), 64), :]

    def p2_copy(r, d):
        return pltpu.make_async_remote_copy(
            src_ref=Y.at[r, d // 2, d % 2], dst_ref=p2_rows(mine, r), send_sem=p2s.at[r, d], recv_sem=p2r.at[r, s],
            device_id=(d, m), device_id_type=MESH,
        )

    def p2_from(r, q):
        return pltpu.make_async_remote_copy(
            src_ref=Y.at[r, q // 2, q % 2], dst_ref=p2_rows(group_of(q), r), send_sem=p2s.at[r, q],
            recv_sem=p2r.at[r, q], device_id=(q, m), device_id_type=MESH,
        )

    def p2_own(r):
        return pltpu.make_async_copy(Y.at[r, s // 2, s % 2], p2_rows(mine, r), own2.at[r])

    @pl.loop(0, 32)
    def _(b):
        rows = pl.ds(pl.multiple_of(b * 128, 128), 128)
        moved[rows, :] = hold_rate * mbuf[rows, :] + gbuf[rows, :]

    for r in range(ROUNDS):
        @pl.loop(1, 32)
        def _(k):
            p1_from(r, (s + k) % 32).wait_recv()

        p1_own(r).wait()

        @pl.loop(0, PER)
        def _(j):
            for h in range(2):
                rows = pl.ds(pl.multiple_of(j * 16 + h * 8, 8), 8)
                low, high = merge_halves(R[r, :, 0, rows, :], R[r, :, 1, rows, :])
                X[j, :, 256 * h : 256 * h + 128] = low.reshape(128, 128)
                X[j, :, 256 * h + 128 : 256 * h + 256] = high.reshape(128, 128)
            G[r, j] = dot_t(X[j], X[j])

        for k in range(1, 4):
            x_copy(r, (x + k) % 4, x).start()
        total = G[r, x]
        for k in range(1, 4):
            q = (x + k) % 4
            x_copy(r, q, q).wait_recv()
            total = total + GX[r, q]
        S[r] = total
        z_copy(r).start()
        z_copy(r).wait_recv()
        gram = S[r] + Z[r]
        scale = lax.rsqrt(jnp.sum(jnp.sum(gram * eye, axis=1, keepdims=True), axis=0, keepdims=True) + 1e-06)
        gram = gram * (scale * scale)
        factor = None
        for step in range(ITERS):
            mixed = 3.4445 * eye + (-4.775 * gram + 2.0315 * dot(gram, gram))
            factor = mixed if factor is None else dot(mixed, factor)
            if step < ITERS - 1:
                gram = dot(dot(mixed, gram), mixed)
        QR[r, x] = factor * scale
        for k in range(1, 4):
            q_copy(r, (x + k) % 4, x).start()
        for k in range(1, 4):
            q = (x + k) % 4
            q_copy(r, q, q).wait_recv()

        @pl.loop(0, PER)
        def _(j):
            for h in range(2):
                wide = dot(QR[r, j], X[j, :, 256 * h : 256 * h + 256])
                rows = pl.ds(pl.multiple_of(j * 16 + h * 8, 8), 8)
                even, odd = merge_halves(wide[:, :128].reshape(16, 8, 128), wide[:, 128:].reshape(16, 8, 128))
                Y[r, :, 0, rows, :] = even
                Y[r, :, 1, rows, :] = odd

        @pl.loop(0, 32)
        def _(k):
            d = dest(k)

            @pl.when(d != s)
            def _():
                p2_copy(r, d).start()

        p2_own(r).start()

    for r in range(ROUNDS):
        p2_own(r).wait()
        z_copy(r).wait_send()
        for k in range(1, 4):
            x_copy(r, (x + k) % 4, x).wait_send()
            q_copy(r, (x + k) % 4, x).wait_send()

        @pl.loop(1, 32)
        def _(k):
            q = (s + k) % 32
            p1_copy(r, q).wait_send()
            p2_copy(r, q).wait_send()

    for r in range(ROUNDS):
        @pl.loop(1, 32)
        def _(k):
            p2_from(r, (s + k) % 32).wait_recv()


def exchange(g, m):
    dma = pltpu.SemaphoreType.DMA
    return pl.pallas_call(
        kernel,
        out_shape=[jax.ShapeDtypeStruct((4096, 128), F32)] * 2,
        in_specs=[pl.BlockSpec(memory_space=pltpu.HBM)] * 2,
        out_specs=[pl.BlockSpec(memory_space=pltpu.VMEM)] * 2,
        scratch_shapes=[
            pltpu.VMEM((4096, 128), F32),
            pltpu.VMEM((4096, 128), F32),
            pltpu.VMEM((4096, 128), F32),
            pltpu.VMEM((ROUNDS, 16, 2, 64, 128), F32),
            pltpu.VMEM((PER, 128, 512), F32),
            pltpu.VMEM((ROUNDS, PER, 128, 128), F32),
            pltpu.VMEM((ROUNDS, 4, 128, 128), F32),
            pltpu.VMEM((ROUNDS, 128, 128), F32),
            pltpu.VMEM((ROUNDS, 128, 128), F32),
            pltpu.VMEM((ROUNDS, 4, 128, 128), F32),
            pltpu.VMEM((ROUNDS, 16, 2, 64, 128), F32),
            dma((4,)), dma((4,)),
            dma((ROUNDS, 32)), dma((ROUNDS, 32)),
            dma((ROUNDS, 4)), dma((ROUNDS, 4)),
            dma((ROUNDS,)), dma((ROUNDS,)),
            dma((ROUNDS, 4)), dma((ROUNDS, 4)),
            dma((ROUNDS, 32)), dma((ROUNDS, 32)),
            dma((ROUNDS,)), dma((ROUNDS,)),
        ],
        compiler_params=pltpu.CompilerParams(
            collective_id=0, has_side_effects=True, vmem_limit_bytes=40 * 1024 * 1024
        ),
        name="exchange",
    )(g, m)


def finish_kernel(w, back, moved, new_w, new_m, held, wsem, msem):
    momentum_out = pltpu.make_async_copy(moved, new_m, msem)
    momentum_out.start()
    pieces = 8
    size = w.shape[0] // pieces
    outs = []
    for i in range(pieces):
        part = pl.ds(i * size, size)

        @pl.loop(0, size // 128)
        def _(b):
            rows = pl.ds(pl.multiple_of(i * size + b * 128, 128), 128)
            held[rows, :] = w[rows, :] - learn_rate * back[rows, :]

        outs.append(pltpu.make_async_copy(held.at[part], new_w.at[part], wsem.at[i]))
        outs[-1].start()
    for out in outs:
        out.wait()
    momentum_out.wait()


def finish(w, back, moved):
    return pl.pallas_call(
        finish_kernel,
        out_shape=[jax.ShapeDtypeStruct(w.shape, F32)] * 2,
        in_specs=[pl.BlockSpec(memory_space=pltpu.VMEM)] * 3,
        out_specs=[pl.BlockSpec(memory_space=pltpu.HBM)] * 2,
        scratch_shapes=[
            pltpu.VMEM(w.shape, F32),
            pltpu.SemaphoreType.DMA((8,)),
            pltpu.SemaphoreType.DMA(()),
        ],
        compiler_params=pltpu.CompilerParams(vmem_limit_bytes=16 * 1024 * 1024),
        name="finish",
    )(w, back, moved)


def flat(a):
    return a.reshape(256, 4, 4, 128).transpose(0, 2, 1, 3).reshape(4096, 128)


def unflat(a):
    return a.reshape(256, 4, 4, 128).transpose(0, 2, 1, 3).reshape(256, 4, 512)


def local(gradients, momentum, weights):
    g, m, w = flat(gradients), flat(momentum), flat(weights)
    new_weights, new_momentum = finish(w, *exchange(*(pltpu.with_memory_space_constraint(a, pltpu.HBM) for a in (g, m))))
    return (unflat(new_weights), unflat(new_momentum))


def solution(mesh):
    placed = P(None, "shard", "model")
    return jax.shard_map(
        local, mesh=mesh, in_specs=(placed,) * 3, out_specs=(placed, placed), check_vma=False
    )
```

```python
import contextlib

import jax
import jax.numpy as jnp
from jax import lax
from jax.experimental import pallas as pl
from jax.experimental.pallas import tpu as pltpu
from jax.sharding import PartitionSpec as P

MESH = pl.DeviceIdType.MESH
F32 = jnp.float32
ITERS = 4
ROUNDS = 2
PER = 4
BLOCKS = (16, 2, ROUNDS, 64, 128)
hold_rate = 0.9
learn_rate = 0.8
HI = lax.Precision.HIGHEST


def scope(name):
    return contextlib.nullcontext()


def dot(a, b):
    return lax.dot_general(a, b, (((1,), (0,)), ((), ())), precision=HI, preferred_element_type=F32)


def dot_t(a, b):
    return lax.dot_general(a, b, (((1,), (1,)), ((), ())), precision=HI, preferred_element_type=F32)


def merge_halves(a, b):
    low = lax.broadcasted_iota(jnp.int32, a.shape, 1) < 4
    return (
        jnp.where(low, a, pltpu.roll(b, 4, 1)),
        jnp.where(low, pltpu.roll(a, 4, 1), b),
    )


def remote(src, dst, send, recv, to):
    return pltpu.make_async_remote_copy(
        src_ref=src, dst_ref=dst, send_sem=send, recv_sem=recv, device_id=to, device_id_type=MESH
    )


def wait_bytes(ref, sem):
    pltpu.make_async_copy(ref, ref, sem).wait()


def kernel(
    g_hbm, m_hbm, back, moved,
    gbuf, mbuf, D, R, X, G, GX, S, Z, QR, Y,
    gsem, msem, p1s, p1r, xs, xr, zs, zr, qs, qr, p2s, p2r, ready,
):
    s, m = lax.axis_index("shard"), lax.axis_index("model")
    zl, yy, core = s // 8, (s // 2) % 4, s % 2
    zh, x = m // 4, m % 4
    side = zl // 2

    loads = []
    for q in range(4):
        c, r = 1 - q % 2, q // 2
        loads.append((
            pltpu.make_async_copy(g_hbm.at[:, c, r], gbuf.at[q], gsem.at[q]),
            pltpu.make_async_copy(m_hbm.at[:, c, r], mbuf.at[q], msem.at[q]),
        ))
        loads[-1][0].start()
        loads[-1][1].start()

    def group_of(d):
        z = d // 8
        return (zh * (3 - z) + (1 - zh) * z) * 8 + d % 8

    mine = group_of(s)
    partner = ((3 - zl) * 8 + s % 8, (1 - zh) * 4 + x)

    def dest(c, k):
        a, b = k // 4, k % 4
        z = side * a + (1 - side) * (3 - a)
        return z * 8 + ((yy + 2 + b) % 4) * 2 + c

    barrier = pltpu.get_barrier_semaphore()

    @pl.when(zh == 0)
    def _():
        pl.semaphore_signal(barrier, inc=1, device_id=partner, device_id_type=MESH)

    @pl.loop(1, 32)
    def _(k):
        pl.semaphore_signal(barrier, inc=1, device_id=((s + k) % 32, m), device_id_type=MESH)

    for k in range(1, 4):
        pl.semaphore_signal(barrier, inc=1, device_id=(s, zh * 4 + (x + k) % 4), device_id_type=MESH)

    for q in range(4):
        c, r = 1 - q % 2, q // 2
        with scope(f"load#q={q}"):
            loads[q][0].wait()
            loads[q][1].wait()

            @pl.loop(0, 8)
            def _(b):
                both = pl.ds(b * 2, 2)
                g = gbuf[q, both]
                D[q, both] = hold_rate * (hold_rate * mbuf[q, both] + g) + g

        if q == 0:
            with scope("barrier"):
                pl.semaphore_wait(barrier, 34 + zh)

            @pl.when(zh == 1)
            def _():
                pl.semaphore_signal(ready, inc=1, device_id=partner, device_id_type=MESH)

        with scope(f"p1send#q={q}"):
            @pl.loop(0, 16)
            def _(k):
                d = dest(c, k)
                rows = D.at[q, group_of(d) // 2]
                place = R.at[r, s // 2, s % 2]

                @pl.when(d != s)
                def _():
                    remote(rows, place, p1s.at[r], p1r.at[r], (d, m)).start()

                @pl.when(d == s)
                def _():
                    pltpu.make_async_copy(rows, place, p1r.at[r]).start()

    with scope("moved"):
        for q in range(4):
            c, r = 1 - q % 2, q // 2

            @pl.loop(0, 8)
            def _(b):
                both = pl.ds(b * 2, 2)
                moved[both, c, r] = hold_rate * mbuf[q, both] + gbuf[q, both]

    eye = (
        lax.broadcasted_iota(jnp.int32, (128, 128), 0) == lax.broadcasted_iota(jnp.int32, (128, 128), 1)
    ).astype(F32)

    for r in range(ROUNDS):
        with scope(f"p1wait#r={r}"):
            wait_bytes(R.at[r], p1r.at[r])

        with scope(f"gram#r={r}"):
            @pl.loop(0, PER)
            def _(j):
                for h in range(2):
                    rows = pl.ds(pl.multiple_of(j * 16 + h * 8, 8), 8)
                    low, high = merge_halves(R[r, :, 0, rows, :], R[r, :, 1, rows, :])
                    X[j, :, 256 * h : 256 * h + 128] = low.reshape(128, 128)
                    X[j, :, 256 * h + 128 : 256 * h + 256] = high.reshape(128, 128)
                G[r, j] = dot_t(X[j], X[j])

        with scope(f"xred#r={r}"):
            for k in range(1, 4):
                q = (x + k) % 4
                remote(G.at[r, q], GX.at[r, 3 - k], xs.at[r], xr.at[r], (s, zh * 4 + q)).start()
            wait_bytes(GX.at[r], xr.at[r])
            S[r] = G[r, x] + GX[r, 0] + GX[r, 1] + GX[r, 2]

        with scope(f"zred#r={r}"):
            if r == 0:
                @pl.when(zh == 0)
                def _():
                    pl.semaphore_wait(ready, 1)

            across = remote(S.at[r], Z.at[r], zs.at[r], zr.at[r], partner)
            across.start()
            across.wait_recv()

        with scope(f"chain#r={r}"):
            gram = S[r] + Z[r]
            scale = lax.rsqrt(jnp.sum(jnp.sum(gram * eye, axis=1, keepdims=True), axis=0, keepdims=True) + 1e-06)
            gram = gram * (scale * scale)
            factor = None
            for step in range(ITERS):
                mixed = 3.4445 * eye + (-4.775 * gram + 2.0315 * dot(gram, gram))
                factor = mixed if factor is None else dot(mixed, factor)
                if step < ITERS - 1:
                    gram = dot(dot(mixed, gram), mixed)
            QR[r, x] = factor * scale

        with scope(f"qcast#r={r}"):
            for k in range(1, 4):
                to = (s, zh * 4 + (x + k) % 4)
                remote(QR.at[r, x], QR.at[r, x], qs.at[r], qr.at[r], to).start()
            wait_bytes(GX.at[r], qr.at[r])

        with scope(f"apply#r={r}"):
            @pl.loop(0, PER)
            def _(j):
                for h in range(2):
                    wide = dot(QR[r, j], X[j, :, 256 * h : 256 * h + 256])
                    rows = pl.ds(pl.multiple_of(j * 16 + h * 8, 8), 8)
                    even, odd = merge_halves(wide[:, :128].reshape(16, 8, 128), wide[:, 128:].reshape(16, 8, 128))
                    Y[r, :, 0, rows, :] = even
                    Y[r, :, 1, rows, :] = odd

        with scope(f"p2send#r={r}"):
            for c in (1, 0):
                @pl.loop(0, 16)
                def _(k):
                    d = dest(c, k)
                    rows = Y.at[r, d // 2, c]
                    place = back.at[mine // 2, mine % 2, r]

                    @pl.when(d != s)
                    def _():
                        remote(rows, place, p2s.at[r], p2r.at[r], (d, m)).start()

                    @pl.when(d == s)
                    def _():
                        pltpu.make_async_copy(rows, place, p2r.at[r]).start()

    with scope("sendwait"):
        for r in range(ROUNDS):
            three = GX.at[r]
            wait_bytes(three, xs.at[r])
            wait_bytes(three, qs.at[r])
            wait_bytes(S.at[r], zs.at[r])
            for sem in (p1s, p2s):
                wait_bytes(Y.at[r, pl.ds(0, 15)], sem.at[r])
                wait_bytes(Y.at[r, 15, 0], sem.at[r])

    for r in range(ROUNDS):
        with scope(f"p2wait#r={r}"):
            wait_bytes(R.at[r], p2r.at[r])


def exchange(g, m):
    dma = pltpu.SemaphoreType.DMA
    quarters = pltpu.VMEM((4, 16, 64, 128), F32)
    moving = pltpu.VMEM((ROUNDS, 16, 2, 64, 128), F32)
    square = (128, 128)
    return pl.pallas_call(
        kernel,
        out_shape=[jax.ShapeDtypeStruct(BLOCKS, F32)] * 2,
        in_specs=[pl.BlockSpec(memory_space=pltpu.HBM)] * 2,
        out_specs=[pl.BlockSpec(memory_space=pltpu.VMEM)] * 2,
        scratch_shapes=[
            quarters, quarters, quarters,
            moving,
            pltpu.VMEM((PER, 128, 512), F32),
            pltpu.VMEM((ROUNDS, PER, *square), F32),
            pltpu.VMEM((ROUNDS, 3, *square), F32),
            pltpu.VMEM((ROUNDS, *square), F32),
            pltpu.VMEM((ROUNDS, *square), F32),
            pltpu.VMEM((ROUNDS, PER, *square), F32),
            moving,
            dma((4,)), dma((4,)),
            *[dma((ROUNDS,))] * 10,
            pltpu.SemaphoreType.REGULAR,
        ],
        compiler_params=pltpu.CompilerParams(
            collective_id=0, has_side_effects=True, vmem_limit_bytes=40 * 1024 * 1024
        ),
        name="exchange",
    )(g, m)


def finish_kernel(w, back, moved, new_w, new_m, held, wsem, msem):
    momentum_out = pltpu.make_async_copy(moved, new_m, msem)
    momentum_out.start()
    pieces = 8
    size = w.shape[0] // pieces
    outs = []
    for i in range(pieces):
        part = pl.ds(i * size, size)

        @pl.loop(0, size // 128)
        def _(b):
            rows = pl.ds(pl.multiple_of(i * size + b * 128, 128), 128)
            held[rows, :] = w[rows, :] - learn_rate * back[rows, :]

        outs.append(pltpu.make_async_copy(held.at[part], new_w.at[part], wsem.at[i]))
        outs[-1].start()
    for out in outs:
        out.wait()
    momentum_out.wait()


def finish(w, back, moved):
    return pl.pallas_call(
        finish_kernel,
        out_shape=[jax.ShapeDtypeStruct(w.shape, F32)] * 2,
        in_specs=[pl.BlockSpec(memory_space=pltpu.VMEM)] * 3,
        out_specs=[pl.BlockSpec(memory_space=pltpu.HBM)] * 2,
        scratch_shapes=[
            pltpu.VMEM(w.shape, F32),
            pltpu.SemaphoreType.DMA((8,)),
            pltpu.SemaphoreType.DMA(()),
        ],
        compiler_params=pltpu.CompilerParams(vmem_limit_bytes=16 * 1024 * 1024),
        name="finish",
    )(w, back, moved)


def flat(a):
    return a.reshape(256, 4, 4, 128).transpose(0, 2, 1, 3).reshape(4096, 128)


def unflat(a):
    return a.reshape(256, 4, 4, 128).transpose(0, 2, 1, 3).reshape(256, 4, 512)


def local(gradients, momentum, weights):
    g, m, w = flat(gradients), flat(momentum), flat(weights)
    inputs = [pltpu.with_memory_space_constraint(a.reshape(BLOCKS), pltpu.HBM) for a in (g, m)]
    back, moved = (a.reshape(4096, 128) for a in exchange(*inputs))
    new_weights, new_momentum = finish(w, back, moved)
    return (unflat(new_weights), unflat(new_momentum))


def solution(mesh):
    placed = P(None, "shard", "model")
    return jax.shard_map(
        local, mesh=mesh, in_specs=(placed,) * 3, out_specs=(placed, placed), check_vma=False
    )
```

```python
import contextlib

import jax
import jax.numpy as jnp
from jax import lax
from jax.experimental import pallas as pl
from jax.experimental.pallas import tpu as pltpu
from jax.sharding import PartitionSpec as P

MESH = pl.DeviceIdType.MESH
F32 = jnp.float32
ITERS = 4
ROUNDS = 2
PER = 4
BLOCKS = (16, 2, ROUNDS, 64, 128)
hold_rate = 0.9
learn_rate = 0.8
HI = lax.Precision.HIGHEST


def scope(name):
    return contextlib.nullcontext()


def dot(a, b):
    return lax.dot_general(a, b, (((1,), (0,)), ((), ())), precision=HI, preferred_element_type=F32)


def dot_t(a, b):
    return lax.dot_general(a, b, (((1,), (1,)), ((), ())), precision=HI, preferred_element_type=F32)


def merge_halves(a, b):
    low = lax.broadcasted_iota(jnp.int32, a.shape, 1) < 4
    return (
        jnp.where(low, a, pltpu.roll(b, 4, 1)),
        jnp.where(low, pltpu.roll(a, 4, 1), b),
    )


def remote(src, dst, send, recv, to):
    return pltpu.make_async_remote_copy(
        src_ref=src, dst_ref=dst, send_sem=send, recv_sem=recv, device_id=to, device_id_type=MESH
    )


def wait_bytes(ref, sem):
    pltpu.make_async_copy(ref, ref, sem).wait()


def kernel(
    g_hbm, m_hbm, back, moved,
    gbuf, mbuf, D, R, X, G, GX, S, Z, QR, Y,
    gsem, msem, p1s, p1r, xs, xr, zs, zr, qs, qr, p2s, p2r, ready,
):
    s, m = lax.axis_index("shard"), lax.axis_index("model")
    zl, yy, core = s // 8, (s // 2) % 4, s % 2
    zh, x = m // 4, m % 4
    side = zl // 2

    def group_of(d):
        z = d // 8
        return (zh * (3 - z) + (1 - zh) * z) * 8 + d % 8

    mine = group_of(s)
    partner = ((3 - zl) * 8 + s % 8, (1 - zh) * 4 + x)

    def dest(c, k):
        a, b = k // 4, k % 4
        z = side * a + (1 - side) * (3 - a)
        return z * 8 + ((yy + 2 + b) % 4) * 2 + c

    barrier = pltpu.get_barrier_semaphore()

    @pl.when(zh == 0)
    def _():
        pl.semaphore_signal(barrier, inc=1, device_id=partner, device_id_type=MESH)

    for k in (16, 24, 8):
        for i in range(8):
            pl.semaphore_signal(barrier, inc=1, device_id=((s + k + i) % 32, m), device_id_type=MESH)
    for k in range(1, 8):
        pl.semaphore_signal(barrier, inc=1, device_id=((s + k) % 32, m), device_id_type=MESH)
    for k in range(1, 4):
        pl.semaphore_signal(barrier, inc=1, device_id=(s, zh * 4 + (x + k) % 4), device_id_type=MESH)

    loads = []
    for q in range(4):
        c, r = 1 - q % 2, q // 2
        loads.append((
            pltpu.make_async_copy(g_hbm.at[:, c, r], gbuf.at[q], gsem.at[q]),
            pltpu.make_async_copy(m_hbm.at[:, c, r], mbuf.at[q], msem.at[q]),
        ))
        loads[-1][0].start()
        loads[-1][1].start()


    for q in range(4):
        c, r = 1 - q % 2, q // 2
        with scope(f"load#q={q}"):
            loads[q][0].wait()
            loads[q][1].wait()

            @pl.loop(0, 8)
            def _(b):
                both = pl.ds(b * 2, 2)
                g = gbuf[q, both]
                D[q, both] = hold_rate * (hold_rate * mbuf[q, both] + g) + g

        if q == 0:
            with scope("barrier"):
                pl.semaphore_wait(barrier, 34 + zh)

            @pl.when(zh == 1)
            def _():
                pl.semaphore_signal(ready, inc=1, device_id=partner, device_id_type=MESH)

        with scope(f"p1send#q={q}"):
            @pl.loop(0, 16)
            def _(k):
                d = dest(c, k)
                rows = D.at[q, group_of(d) // 2]
                place = R.at[r, s // 2, s % 2]

                @pl.when(d != s)
                def _():
                    remote(rows, place, p1s.at[r], p1r.at[r], (d, m)).start()

                @pl.when(d == s)
                def _():
                    pltpu.make_async_copy(rows, place, p1r.at[r]).start()

    with scope("moved"):
        for q in range(4):
            c, r = 1 - q % 2, q // 2

            @pl.loop(0, 8)
            def _(b):
                both = pl.ds(b * 2, 2)
                moved[both, c, r] = hold_rate * mbuf[q, both] + gbuf[q, both]

    eye = (
        lax.broadcasted_iota(jnp.int32, (128, 128), 0) == lax.broadcasted_iota(jnp.int32, (128, 128), 1)
    ).astype(F32)

    def gram_step(r):
        with scope(f"p1wait#r={r}"):
            wait_bytes(R.at[r], p1r.at[r])

        with scope(f"gram#r={r}"):
            @pl.loop(0, PER)
            def _(j):
                for h in range(2):
                    rows = pl.ds(pl.multiple_of(j * 16 + h * 8, 8), 8)
                    low, high = merge_halves(R[r, :, 0, rows, :], R[r, :, 1, rows, :])
                    X[r, j, :, 256 * h : 256 * h + 128] = low.reshape(128, 128)
                    X[r, j, :, 256 * h + 128 : 256 * h + 256] = high.reshape(128, 128)
                G[r, j] = dot_t(X[r, j], X[r, j])

            for k in range(1, 4):
                q = (x + k) % 4
                remote(G.at[r, q], GX.at[r, 3 - k], xs.at[r], xr.at[r], (s, zh * 4 + q)).start()

    def sum_step(r):
        with scope(f"xred#r={r}"):
            wait_bytes(GX.at[r], xr.at[r])
            S[r] = G[r, x] + GX[r, 0] + GX[r, 1] + GX[r, 2]
            if r == 0:
                @pl.when(zh == 0)
                def _():
                    pl.semaphore_wait(ready, 1)

            remote(S.at[r], Z.at[r], zs.at[r], zr.at[r], partner).start()

    def chain_step(r):
        with scope(f"zred#r={r}"):
            remote(S.at[r], Z.at[r], zs.at[r], zr.at[r], partner).wait_recv()

        with scope(f"chain#r={r}"):
            gram = S[r] + Z[r]
            scale = lax.rsqrt(jnp.sum(jnp.sum(gram * eye, axis=1, keepdims=True), axis=0, keepdims=True) + 1e-06)
            gram = gram * (scale * scale)
            factor = None
            for step in range(ITERS):
                mixed = 3.4445 * eye + (-4.775 * gram + 2.0315 * dot(gram, gram))
                factor = mixed if factor is None else dot(mixed, factor)
                if step < ITERS - 1:
                    gram = dot(dot(mixed, gram), mixed)
            QR[r, x] = factor * scale
            for k in range(1, 4):
                to = (s, zh * 4 + (x + k) % 4)
                remote(QR.at[r, x], QR.at[r, x], qs.at[r], qr.at[r], to).start()

    def apply_step(r):
        with scope(f"qcast#r={r}"):
            wait_bytes(GX.at[r], qr.at[r])

        with scope(f"apply#r={r}"):
            @pl.loop(0, PER)
            def _(j):
                for h in range(2):
                    wide = dot(QR[r, j], X[r, j, :, 256 * h : 256 * h + 256])
                    rows = pl.ds(pl.multiple_of(j * 16 + h * 8, 8), 8)
                    even, odd = merge_halves(wide[:, :128].reshape(16, 8, 128), wide[:, 128:].reshape(16, 8, 128))
                    Y[r, :, 0, rows, :] = even
                    Y[r, :, 1, rows, :] = odd

        with scope(f"p2send#r={r}"):
            for c in (1, 0):
                @pl.loop(0, 16)
                def _(k):
                    d = dest(c, k)
                    rows = Y.at[r, d // 2, c]
                    place = back.at[mine // 2, mine % 2, r]

                    @pl.when(d != s)
                    def _():
                        remote(rows, place, p2s.at[r], p2r.at[r], (d, m)).start()

                    @pl.when(d == s)
                    def _():
                        pltpu.make_async_copy(rows, place, p2r.at[r]).start()

    gram_step(0)
    sum_step(0)
    chain_step(0)

    @pl.when(zh == 1)
    def _():
        gram_step(1)

    apply_step(0)

    @pl.when(jnp.logical_not(zh == 1))
    def _():
        gram_step(1)

    sum_step(1)
    chain_step(1)
    apply_step(1)
    with scope("sendwait"):
        for r in range(ROUNDS):
            three = GX.at[r]
            wait_bytes(three, xs.at[r])
            wait_bytes(three, qs.at[r])
            wait_bytes(S.at[r], zs.at[r])
            for sem in (p1s, p2s):
                wait_bytes(Y.at[r, pl.ds(0, 15)], sem.at[r])
                wait_bytes(Y.at[r, 15, 0], sem.at[r])

    for r in range(ROUNDS):
        with scope(f"p2wait#r={r}"):
            wait_bytes(R.at[r], p2r.at[r])


def exchange(g, m):
    dma = pltpu.SemaphoreType.DMA
    quarters = pltpu.VMEM((4, 16, 64, 128), F32)
    moving = pltpu.VMEM((ROUNDS, 16, 2, 64, 128), F32)
    square = (128, 128)
    return pl.pallas_call(
        kernel,
        out_shape=[jax.ShapeDtypeStruct(BLOCKS, F32)] * 2,
        in_specs=[pl.BlockSpec(memory_space=pltpu.HBM)] * 2,
        out_specs=[pl.BlockSpec(memory_space=pltpu.VMEM)] * 2,
        scratch_shapes=[
            quarters, quarters, quarters,
            moving,
            pltpu.VMEM((ROUNDS, PER, 128, 512), F32),
            pltpu.VMEM((ROUNDS, PER, *square), F32),
            pltpu.VMEM((ROUNDS, 3, *square), F32),
            pltpu.VMEM((ROUNDS, *square), F32),
            pltpu.VMEM((ROUNDS, *square), F32),
            pltpu.VMEM((ROUNDS, PER, *square), F32),
            moving,
            dma((4,)), dma((4,)),
            *[dma((ROUNDS,))] * 10,
            pltpu.SemaphoreType.REGULAR,
        ],
        compiler_params=pltpu.CompilerParams(
            collective_id=0, has_side_effects=True, vmem_limit_bytes=40 * 1024 * 1024
        ),
        name="exchange",
    )(g, m)


def finish_kernel(w, back, moved, new_w, new_m, held, wsem, msem):
    momentum_out = pltpu.make_async_copy(moved, new_m, msem)
    momentum_out.start()
    pieces = 8
    size = w.shape[0] // pieces
    outs = []
    for i in range(pieces):
        part = pl.ds(i * size, size)

        @pl.loop(0, size // 128)
        def _(b):
            rows = pl.ds(pl.multiple_of(i * size + b * 128, 128), 128)
            held[rows, :] = w[rows, :] - learn_rate * back[rows, :]

        outs.append(pltpu.make_async_copy(held.at[part], new_w.at[part], wsem.at[i]))
        outs[-1].start()
    for out in outs:
        out.wait()
    momentum_out.wait()


def finish(w, back, moved):
    return pl.pallas_call(
        finish_kernel,
        out_shape=[jax.ShapeDtypeStruct(w.shape, F32)] * 2,
        in_specs=[pl.BlockSpec(memory_space=pltpu.VMEM)] * 3,
        out_specs=[pl.BlockSpec(memory_space=pltpu.HBM)] * 2,
        scratch_shapes=[
            pltpu.VMEM(w.shape, F32),
            pltpu.SemaphoreType.DMA((8,)),
            pltpu.SemaphoreType.DMA(()),
        ],
        compiler_params=pltpu.CompilerParams(vmem_limit_bytes=16 * 1024 * 1024),
        name="finish",
    )(w, back, moved)


def flat(a):
    return a.reshape(256, 4, 4, 128).transpose(0, 2, 1, 3).reshape(4096, 128)


def unflat(a):
    return a.reshape(256, 4, 4, 128).transpose(0, 2, 1, 3).reshape(256, 4, 512)


def local(gradients, momentum, weights):
    g, m, w = flat(gradients), flat(momentum), flat(weights)
    inputs = [pltpu.with_memory_space_constraint(a.reshape(BLOCKS), pltpu.HBM) for a in (g, m)]
    back, moved = (a.reshape(4096, 128) for a in exchange(*inputs))
    new_weights, new_momentum = finish(w, back, moved)
    return (unflat(new_weights), unflat(new_momentum))


def solution(mesh):
    placed = P(None, "shard", "model")
    return jax.shard_map(
        local, mesh=mesh, in_specs=(placed,) * 3, out_specs=(placed, placed), check_vma=False
    )
```

```python
import contextlib

import jax
import jax.numpy as jnp
from jax import lax
from jax.experimental import pallas as pl
from jax.experimental.pallas import tpu as pltpu
from jax.sharding import PartitionSpec as P

MESH = pl.DeviceIdType.MESH
F32 = jnp.float32
ITERS = 4
ROUNDS = 2
PER = 4
BLOCKS = (16, 2, ROUNDS, 64, 128)
hold_rate = 0.9
learn_rate = 0.8
HI = lax.Precision.HIGHEST


def scope(name):
    return contextlib.nullcontext()


def dot(a, b):
    return lax.dot_general(a, b, (((1,), (0,)), ((), ())), precision=HI, preferred_element_type=F32)


def dot_t(a, b):
    return lax.dot_general(a, b, (((1,), (1,)), ((), ())), precision=HI, preferred_element_type=F32)


def merge_halves(a, b):
    low = lax.broadcasted_iota(jnp.int32, a.shape, 1) < 4
    return (
        jnp.where(low, a, pltpu.roll(b, 4, 1)),
        jnp.where(low, pltpu.roll(a, 4, 1), b),
    )


def remote(src, dst, send, recv, to):
    return pltpu.make_async_remote_copy(
        src_ref=src, dst_ref=dst, send_sem=send, recv_sem=recv, device_id=to, device_id_type=MESH
    )


def wait_bytes(ref, sem):
    pltpu.make_async_copy(ref, ref, sem).wait()


def kernel(
    g_hbm, m_hbm, w_hbm, back, moved, held_w,
    gbuf, mbuf, D, R, X, G, GX, S, Z, QR, Y,
    wsem, gsem, msem, p1s, p1r, xs, xr, zs, zr, qs, qr, p2s, p2r, ready,
):
    s, m = lax.axis_index("shard"), lax.axis_index("model")
    zl, yy, core = s // 8, (s // 2) % 4, s % 2
    zh, x = m // 4, m % 4
    side = zl // 2

    loads = []
    for q in range(4):
        c, r = 1 - q % 2, q // 2
        loads.append((
            pltpu.make_async_copy(g_hbm.at[:, c, r], gbuf.at[q], gsem.at[q]),
            pltpu.make_async_copy(m_hbm.at[:, c, r], mbuf.at[q], msem.at[q]),
        ))

    def load(q):
        for copy in loads[q]:
            copy.start()

    load(0)

    def group_of(d):
        z = d // 8
        return (zh * (3 - z) + (1 - zh) * z) * 8 + d % 8

    mine = group_of(s)
    partner = ((3 - zl) * 8 + s % 8, (1 - zh) * 4 + x)

    def dest(c, k):
        a, b = k // 4, k % 4
        z = side * a + (1 - side) * (3 - a)
        return z * 8 + ((yy + 2 + b) % 4) * 2 + c

    def late_dest(c, k):
        half, a, b = k // 8, (k % 8) // 2, k % 2
        z = side * a + (1 - side) * (3 - a)
        return z * 8 + (half * 2 + (yy + 1 + b) % 2) * 2 + c

    barrier = pltpu.get_barrier_semaphore()

    @pl.when(zh == 0)
    def _():
        pl.semaphore_signal(barrier, inc=1, device_id=partner, device_id_type=MESH)

    for k in (16, 24, 8):
        for i in range(8):
            pl.semaphore_signal(barrier, inc=1, device_id=((s + k + i) % 32, m), device_id_type=MESH)
    for k in range(1, 8):
        pl.semaphore_signal(barrier, inc=1, device_id=((s + k) % 32, m), device_id_type=MESH)
    for k in range(1, 4):
        pl.semaphore_signal(barrier, inc=1, device_id=(s, zh * 4 + (x + k) % 4), device_id_type=MESH)


    for q in range(4):
        c, r = 1 - q % 2, q // 2
        with scope(f"load#q={q}"):
            for copy in loads[q]:
                copy.wait()
            if q == 0:
                for later in range(1, 4):
                    load(later)

            @pl.loop(0, 8)
            def _(b):
                both = pl.ds(b * 2, 2)
                g = gbuf[q, both]
                D[q, both] = hold_rate * (hold_rate * mbuf[q, both] + g) + g

        if q == 0:
            with scope("barrier"):
                pl.semaphore_wait(barrier, 34 + zh)

            @pl.when(zh == 1)
            def _():
                pl.semaphore_signal(ready, inc=1, device_id=partner, device_id_type=MESH)

        with scope(f"p1send#q={q}"):
            @pl.loop(0, 16)
            def _(k):
                d = dest(c, k)
                rows = D.at[q, group_of(d) // 2]
                place = R.at[r, s // 2, s % 2]

                @pl.when(d != s)
                def _():
                    remote(rows, place, p1s.at[r], p1r.at[r], (d, m)).start()

                @pl.when(d == s)
                def _():
                    pltpu.make_async_copy(rows, place, p1r.at[r]).start()

    pltpu.make_async_copy(w_hbm, held_w, wsem).start()

    with scope("moved"):
        for q in range(4):
            c, r = 1 - q % 2, q // 2

            @pl.loop(0, 8)
            def _(b):
                both = pl.ds(b * 2, 2)
                moved[both, c, r] = hold_rate * mbuf[q, both] + gbuf[q, both]

    eye = (
        lax.broadcasted_iota(jnp.int32, (128, 128), 0) == lax.broadcasted_iota(jnp.int32, (128, 128), 1)
    ).astype(F32)

    def gram_step(r):
        with scope(f"p1wait#r={r}"):
            wait_bytes(R.at[r], p1r.at[r])

        with scope(f"gram#r={r}"):
            @pl.loop(0, PER)
            def _(j):
                for h in range(2):
                    rows = pl.ds(pl.multiple_of(j * 16 + h * 8, 8), 8)
                    low, high = merge_halves(R[r, :, 0, rows, :], R[r, :, 1, rows, :])
                    X[r, j, :, 256 * h : 256 * h + 128] = low.reshape(128, 128)
                    X[r, j, :, 256 * h + 128 : 256 * h + 256] = high.reshape(128, 128)
                G[r, j] = dot_t(X[r, j], X[r, j])

            for k in range(1, 4):
                q = (x + k) % 4
                remote(G.at[r, q], GX.at[r, 3 - k], xs.at[r], xr.at[r], (s, zh * 4 + q)).start()

    def sum_step(r):
        with scope(f"xred#r={r}"):
            wait_bytes(GX.at[r], xr.at[r])
            S[r] = G[r, x] + GX[r, 0] + GX[r, 1] + GX[r, 2]
            if r == 0:
                @pl.when(zh == 0)
                def _():
                    pl.semaphore_wait(ready, 1)

            remote(S.at[r], Z.at[r], zs.at[r], zr.at[r], partner).start()

    def chain_step(r):
        with scope(f"zred#r={r}"):
            remote(S.at[r], Z.at[r], zs.at[r], zr.at[r], partner).wait_recv()

        with scope(f"chain#r={r}"):
            gram = S[r] + Z[r]
            scale = lax.rsqrt(jnp.sum(jnp.sum(gram * eye, axis=1, keepdims=True), axis=0, keepdims=True) + 1e-06)
            gram = gram * (scale * scale)
            factor = None
            for step in range(ITERS):
                mixed = 3.4445 * eye + (-4.775 * gram + 2.0315 * dot(gram, gram))
                factor = mixed if factor is None else dot(mixed, factor)
                if step < ITERS - 1:
                    gram = dot(dot(mixed, gram), mixed)
            QR[r, x] = factor * scale
            for k in range(1, 4):
                to = (s, zh * 4 + (x + k) % 4)
                remote(QR.at[r, x], QR.at[r, x], qs.at[r], qr.at[r], to).start()

    def apply_step(r):
        with scope(f"qcast#r={r}"):
            wait_bytes(GX.at[r], qr.at[r])

        with scope(f"apply#r={r}"):
            @pl.loop(0, PER)
            def _(j):
                for h in range(2):
                    wide = dot(QR[r, j], X[r, j, :, 256 * h : 256 * h + 256])
                    rows = pl.ds(pl.multiple_of(j * 16 + h * 8, 8), 8)
                    even, odd = merge_halves(wide[:, :128].reshape(16, 8, 128), wide[:, 128:].reshape(16, 8, 128))
                    Y[r, :, 0, rows, :] = even
                    Y[r, :, 1, rows, :] = odd

        with scope(f"p2send#r={r}"):
            for c in (1, 0):
                @pl.loop(0, 16)
                def _(k):
                    d = late_dest(c, k) if c in (0, 1) else dest(c, k)
                    rows = Y.at[r, d // 2, c]
                    place = back.at[mine // 2, mine % 2, r]

                    @pl.when(d != s)
                    def _():
                        remote(rows, place, p2s.at[r], p2r.at[r], (d, m)).start()

                    @pl.when(d == s)
                    def _():
                        pltpu.make_async_copy(rows, place, p2r.at[r]).start()

    gram_step(0)
    sum_step(0)
    chain_step(0)

    @pl.when(zh == 1)
    def _():
        gram_step(1)

    apply_step(0)

    @pl.when(jnp.logical_not(zh == 1))
    def _():
        gram_step(1)

    sum_step(1)
    chain_step(1)
    apply_step(1)
    with scope("sendwait"):
        pltpu.make_async_copy(w_hbm, held_w, wsem).wait()
        for r in range(ROUNDS):
            three = GX.at[r]
            wait_bytes(three, xs.at[r])
            wait_bytes(three, qs.at[r])
            wait_bytes(S.at[r], zs.at[r])
            for sem in (p1s, p2s):
                wait_bytes(Y.at[r, pl.ds(0, 15)], sem.at[r])
                wait_bytes(Y.at[r, 15, 0], sem.at[r])

    for r in range(ROUNDS):
        with scope(f"p2wait#r={r}"):
            wait_bytes(R.at[r], p2r.at[r])


def exchange(g, m, w):
    dma = pltpu.SemaphoreType.DMA
    quarters = pltpu.VMEM((4, 16, 64, 128), F32)
    moving = pltpu.VMEM((ROUNDS, 16, 2, 64, 128), F32)
    square = (128, 128)
    return pl.pallas_call(
        kernel,
        out_shape=[jax.ShapeDtypeStruct(BLOCKS, F32)] * 3,
        in_specs=[pl.BlockSpec(memory_space=pltpu.HBM)] * 3,
        out_specs=[pl.BlockSpec(memory_space=pltpu.VMEM)] * 3,
        scratch_shapes=[
            quarters, quarters, quarters,
            moving,
            pltpu.VMEM((ROUNDS, PER, 128, 512), F32),
            pltpu.VMEM((ROUNDS, PER, *square), F32),
            pltpu.VMEM((ROUNDS, 3, *square), F32),
            pltpu.VMEM((ROUNDS, *square), F32),
            pltpu.VMEM((ROUNDS, *square), F32),
            pltpu.VMEM((ROUNDS, PER, *square), F32),
            moving,
            dma(()), dma((4,)), dma((4,)),
            *[dma((ROUNDS,))] * 10,
            pltpu.SemaphoreType.REGULAR,
        ],
        compiler_params=pltpu.CompilerParams(
            collective_id=0, has_side_effects=True, vmem_limit_bytes=40 * 1024 * 1024
        ),
        name="exchange",
    )(g, m, w)


def finish_kernel(w, back, moved, new_w, new_m, held, wsem, msem):
    momentum_out = pltpu.make_async_copy(moved, new_m, msem)
    momentum_out.start()
    pieces = 8
    size = w.shape[0] // pieces
    outs = []
    for i in range(pieces):
        part = pl.ds(i * size, size)

        @pl.loop(0, size // 128)
        def _(b):
            rows = pl.ds(pl.multiple_of(i * size + b * 128, 128), 128)
            held[rows, :] = w[rows, :] - learn_rate * back[rows, :]

        outs.append(pltpu.make_async_copy(held.at[part], new_w.at[part], wsem.at[i]))
        outs[-1].start()
    for out in outs:
        out.wait()
    momentum_out.wait()


def finish(w, back, moved):
    return pl.pallas_call(
        finish_kernel,
        out_shape=[jax.ShapeDtypeStruct(w.shape, F32)] * 2,
        in_specs=[pl.BlockSpec(memory_space=pltpu.VMEM)] * 3,
        out_specs=[pl.BlockSpec(memory_space=pltpu.HBM)] * 2,
        scratch_shapes=[
            pltpu.VMEM(w.shape, F32),
            pltpu.SemaphoreType.DMA((8,)),
            pltpu.SemaphoreType.DMA(()),
        ],
        compiler_params=pltpu.CompilerParams(vmem_limit_bytes=16 * 1024 * 1024),
        name="finish",
    )(w, back, moved)


def flat(a):
    return a.reshape(256, 4, 4, 128).transpose(0, 2, 1, 3).reshape(4096, 128)


def unflat(a):
    return a.reshape(256, 4, 4, 128).transpose(0, 2, 1, 3).reshape(256, 4, 512)


def local(gradients, momentum, weights):
    g, m, w = flat(gradients), flat(momentum), flat(weights)
    inputs = [pltpu.with_memory_space_constraint(a.reshape(BLOCKS), pltpu.HBM) for a in (g, m, w)]
    back, moved, w = (a.reshape(4096, 128) for a in exchange(*inputs))
    new_weights, new_momentum = finish(w, back, moved)
    return (unflat(new_weights), unflat(new_momentum))


def solution(mesh):
    placed = P(None, "shard", "model")
    return jax.shard_map(
        local, mesh=mesh, in_specs=(placed,) * 3, out_specs=(placed, placed), check_vma=False
    )
```

```python
import contextlib

import jax
import jax.numpy as jnp
from jax import lax
from jax.experimental import pallas as pl
from jax.experimental.pallas import tpu as pltpu
from jax.sharding import PartitionSpec as P

MESH = pl.DeviceIdType.MESH
F32 = jnp.float32
ITERS = 4
LINEAR = 3.4445
ROUNDS = 2
PER = 4
BLOCKS = (16, 2, ROUNDS, 64, 128)
hold_rate = 0.9
learn_rate = 0.8
HI = lax.Precision.HIGHEST


def scope(name):
    return contextlib.nullcontext()


def dot(a, b):
    return lax.dot_general(a, b, (((1,), (0,)), ((), ())), precision=HI, preferred_element_type=F32)


def dot_t(a, b):
    return lax.dot_general(a, b, (((1,), (1,)), ((), ())), precision=HI, preferred_element_type=F32)


def merge_halves(a, b):
    low = lax.broadcasted_iota(jnp.int32, a.shape, 1) < 4
    return (
        jnp.where(low, a, pltpu.roll(b, 4, 1)),
        jnp.where(low, pltpu.roll(a, 4, 1), b),
    )


def remote(src, dst, send, recv, to):
    return pltpu.make_async_remote_copy(
        src_ref=src, dst_ref=dst, send_sem=send, recv_sem=recv, device_id=to, device_id_type=MESH
    )


def wait_bytes(ref, sem):
    pltpu.make_async_copy(ref, ref, sem).wait()


def kernel(
    g_hbm, m_hbm, w_hbm, back, moved, held_w,
    gbuf, mbuf, D, R, X, G, GX, S, Z, QR, Y,
    wsem, gsem, msem, p1s, p1r, xs, xr, zs, zr, qs, qr, p2s, p2r, ready,
):
    s, m = lax.axis_index("shard"), lax.axis_index("model")
    zl, yy, core = s // 8, (s // 2) % 4, s % 2
    zh, x = m // 4, m % 4
    side = zl // 2

    loads = []
    for q in range(4):
        c, r = 1 - q % 2, q // 2
        loads.append((
            pltpu.make_async_copy(g_hbm.at[:, c, r], gbuf.at[q], gsem.at[q]),
            pltpu.make_async_copy(m_hbm.at[:, c, r], mbuf.at[q], msem.at[q]),
        ))

    def load(q):
        for copy in loads[q]:
            copy.start()

    load(0)

    def group_of(d):
        z = d // 8
        return (zh * (3 - z) + (1 - zh) * z) * 8 + d % 8

    mine = group_of(s)
    partner = ((3 - zl) * 8 + s % 8, (1 - zh) * 4 + x)

    def dest(c, k):
        a, b = k // 4, k % 4
        z = side * a + (1 - side) * (3 - a)
        return z * 8 + ((yy + 2 + b) % 4) * 2 + c

    def late_dest(c, k):
        half, a, b = k // 8, (k % 8) // 2, k % 2
        z = side * a + (1 - side) * (3 - a)
        return z * 8 + (half * 2 + (yy + 1 + b) % 2) * 2 + c

    barrier = pltpu.get_barrier_semaphore()

    @pl.when(zh == 0)
    def _():
        pl.semaphore_signal(barrier, inc=1, device_id=partner, device_id_type=MESH)

    for k in (16, 24, 8):
        for i in range(8):
            pl.semaphore_signal(barrier, inc=1, device_id=((s + k + i) % 32, m), device_id_type=MESH)
    for k in range(1, 8):
        pl.semaphore_signal(barrier, inc=1, device_id=((s + k) % 32, m), device_id_type=MESH)
    for k in range(1, 4):
        pl.semaphore_signal(barrier, inc=1, device_id=(s, zh * 4 + (x + k) % 4), device_id_type=MESH)


    for q in range(4):
        c, r = 1 - q % 2, q // 2
        with scope(f"load#q={q}"):
            for copy in loads[q]:
                copy.wait()
            if q == 0:
                for later in range(1, 4):
                    load(later)

            @pl.loop(0, 8)
            def _(b):
                both = pl.ds(b * 2, 2)
                g = gbuf[q, both]
                D[q, both] = hold_rate * (hold_rate * mbuf[q, both] + g) + g

        if q == 0:
            with scope("barrier"):
                pl.semaphore_wait(barrier, 34 + zh)

            @pl.when(zh == 1)
            def _():
                pl.semaphore_signal(ready, inc=1, device_id=partner, device_id_type=MESH)

        with scope(f"p1send#q={q}"):
            @pl.loop(0, 16)
            def _(k):
                d = dest(c, k)
                rows = D.at[q, group_of(d) // 2]
                place = R.at[r, s // 2, s % 2]

                @pl.when(d != s)
                def _():
                    remote(rows, place, p1s.at[r], p1r.at[r], (d, m)).start()

                @pl.when(d == s)
                def _():
                    pltpu.make_async_copy(rows, place, p1r.at[r]).start()

    pltpu.make_async_copy(w_hbm, held_w, wsem).start()

    with scope("moved"):
        for q in range(4):
            c, r = 1 - q % 2, q // 2

            @pl.loop(0, 8)
            def _(b):
                both = pl.ds(b * 2, 2)
                moved[both, c, r] = hold_rate * mbuf[q, both] + gbuf[q, both]

    eye = (
        lax.broadcasted_iota(jnp.int32, (128, 128), 0) == lax.broadcasted_iota(jnp.int32, (128, 128), 1)
    ).astype(F32)

    def gram_step(r):
        with scope(f"p1wait#r={r}"):
            wait_bytes(R.at[r], p1r.at[r])

        with scope(f"gram#r={r}"):
            @pl.loop(0, PER)
            def _(j):
                for h in range(2):
                    rows = pl.ds(pl.multiple_of(j * 16 + h * 8, 8), 8)
                    low, high = merge_halves(R[r, :, 0, rows, :], R[r, :, 1, rows, :])
                    X[r, j, :, 256 * h : 256 * h + 128] = low.reshape(128, 128)
                    X[r, j, :, 256 * h + 128 : 256 * h + 256] = high.reshape(128, 128)
                G[r, j] = dot_t(X[r, j], X[r, j])

            for k in range(1, 4):
                q = (x + k) % 4
                remote(G.at[r, q], GX.at[r, 3 - k], xs.at[r], xr.at[r], (s, zh * 4 + q)).start()

    def sum_step(r):
        with scope(f"xred#r={r}"):
            wait_bytes(GX.at[r], xr.at[r])
            S[r] = G[r, x] + GX[r, 0] + GX[r, 1] + GX[r, 2]
            if r == 0:
                @pl.when(zh == 0)
                def _():
                    pl.semaphore_wait(ready, 1)

            remote(S.at[r], Z.at[r], zs.at[r], zr.at[r], partner).start()

    def chain_step(r):
        with scope(f"zred#r={r}"):
            remote(S.at[r], Z.at[r], zs.at[r], zr.at[r], partner).wait_recv()

        with scope(f"chain#r={r}"):
            gram = S[r] + Z[r]
            scale = lax.rsqrt(jnp.sum(jnp.sum(gram * eye, axis=1, keepdims=True), axis=0, keepdims=True) + 1e-06)
            gram = gram * (scale * scale)
            n = []
            for step in range(ITERS):
                n.append(-4.775 * gram + 2.0315 * dot(gram, gram))
                if step < ITERS - 1:
                    mixed = LINEAR * eye + n[-1]
                    gram = dot(dot(mixed, gram), mixed)
            early = LINEAR * (n[0] + n[1]) + dot(n[1], n[0])
            late = LINEAR * (n[2] + n[3]) + dot(n[3], n[2])
            QR[r, x] = (LINEAR**4 * eye + (LINEAR**2 * (early + late) + dot(late, early))) * scale
            for k in range(1, 4):
                to = (s, zh * 4 + (x + k) % 4)
                remote(QR.at[r, x], QR.at[r, x], qs.at[r], qr.at[r], to).start()

    def apply_step(r):
        with scope(f"qcast#r={r}"):
            wait_bytes(GX.at[r], qr.at[r])

        with scope(f"apply#r={r}"):
            @pl.loop(0, PER)
            def _(j):
                for h in range(2):
                    wide = dot(QR[r, j], X[r, j, :, 256 * h : 256 * h + 256])
                    rows = pl.ds(pl.multiple_of(j * 16 + h * 8, 8), 8)
                    even, odd = merge_halves(wide[:, :128].reshape(16, 8, 128), wide[:, 128:].reshape(16, 8, 128))
                    Y[r, :, 0, rows, :] = even
                    Y[r, :, 1, rows, :] = odd

        with scope(f"p2send#r={r}"):
            for c in (1, 0):
                @pl.loop(0, 16)
                def _(k):
                    d = late_dest(c, k) if c in (0, 1) else dest(c, k)
                    rows = Y.at[r, d // 2, c]
                    place = back.at[mine // 2, mine % 2, r]

                    @pl.when(d != s)
                    def _():
                        remote(rows, place, p2s.at[r], p2r.at[r], (d, m)).start()

                    @pl.when(d == s)
                    def _():
                        pltpu.make_async_copy(rows, place, p2r.at[r]).start()

    gram_step(0)
    sum_step(0)
    chain_step(0)

    @pl.when(zh == 1)
    def _():
        gram_step(1)

    apply_step(0)

    @pl.when(jnp.logical_not(zh == 1))
    def _():
        gram_step(1)

    sum_step(1)
    chain_step(1)
    apply_step(1)
    with scope("sendwait"):
        pltpu.make_async_copy(w_hbm, held_w, wsem).wait()
        for r in range(ROUNDS):
            three = GX.at[r]
            wait_bytes(three, xs.at[r])
            wait_bytes(three, qs.at[r])
            wait_bytes(S.at[r], zs.at[r])
            for sem in (p1s, p2s):
                wait_bytes(Y.at[r, pl.ds(0, 15)], sem.at[r])
                wait_bytes(Y.at[r, 15, 0], sem.at[r])

    for r in range(ROUNDS):
        with scope(f"p2wait#r={r}"):
            wait_bytes(R.at[r], p2r.at[r])


def exchange(g, m, w):
    dma = pltpu.SemaphoreType.DMA
    quarters = pltpu.VMEM((4, 16, 64, 128), F32)
    moving = pltpu.VMEM((ROUNDS, 16, 2, 64, 128), F32)
    square = (128, 128)
    return pl.pallas_call(
        kernel,
        out_shape=[jax.ShapeDtypeStruct(BLOCKS, F32)] * 3,
        in_specs=[pl.BlockSpec(memory_space=pltpu.HBM)] * 3,
        out_specs=[pl.BlockSpec(memory_space=pltpu.VMEM)] * 3,
        scratch_shapes=[
            quarters, quarters, quarters,
            moving,
            pltpu.VMEM((ROUNDS, PER, 128, 512), F32),
            pltpu.VMEM((ROUNDS, PER, *square), F32),
            pltpu.VMEM((ROUNDS, 3, *square), F32),
            pltpu.VMEM((ROUNDS, *square), F32),
            pltpu.VMEM((ROUNDS, *square), F32),
            pltpu.VMEM((ROUNDS, PER, *square), F32),
            moving,
            dma(()), dma((4,)), dma((4,)),
            *[dma((ROUNDS,))] * 10,
            pltpu.SemaphoreType.REGULAR,
        ],
        compiler_params=pltpu.CompilerParams(
            collective_id=0, has_side_effects=True, vmem_limit_bytes=40 * 1024 * 1024
        ),
        name="exchange",
    )(g, m, w)


def finish_kernel(w, back, moved, new_w, new_m, held, wsem, msem):
    momentum_out = pltpu.make_async_copy(moved, new_m, msem)
    momentum_out.start()
    pieces = 8
    size = w.shape[0] // pieces
    outs = []
    for i in range(pieces):
        part = pl.ds(i * size, size)

        @pl.loop(0, size // 128)
        def _(b):
            rows = pl.ds(pl.multiple_of(i * size + b * 128, 128), 128)
            held[rows, :] = w[rows, :] - learn_rate * back[rows, :]

        outs.append(pltpu.make_async_copy(held.at[part], new_w.at[part], wsem.at[i]))
        outs[-1].start()
    for out in outs:
        out.wait()
    momentum_out.wait()


def finish(w, back, moved):
    return pl.pallas_call(
        finish_kernel,
        out_shape=[jax.ShapeDtypeStruct(w.shape, F32)] * 2,
        in_specs=[pl.BlockSpec(memory_space=pltpu.VMEM)] * 3,
        out_specs=[pl.BlockSpec(memory_space=pltpu.HBM)] * 2,
        scratch_shapes=[
            pltpu.VMEM(w.shape, F32),
            pltpu.SemaphoreType.DMA((8,)),
            pltpu.SemaphoreType.DMA(()),
        ],
        compiler_params=pltpu.CompilerParams(vmem_limit_bytes=16 * 1024 * 1024),
        name="finish",
    )(w, back, moved)


def flat(a):
    return a.reshape(256, 4, 4, 128).transpose(0, 2, 1, 3).reshape(4096, 128)


def unflat(a):
    return a.reshape(256, 4, 4, 128).transpose(0, 2, 1, 3).reshape(256, 4, 512)


def local(gradients, momentum, weights):
    g, m, w = flat(gradients), flat(momentum), flat(weights)
    inputs = [pltpu.with_memory_space_constraint(a.reshape(BLOCKS), pltpu.HBM) for a in (g, m, w)]
    back, moved, w = (a.reshape(4096, 128) for a in exchange(*inputs))
    new_weights, new_momentum = finish(w, back, moved)
    return (unflat(new_weights), unflat(new_momentum))


def solution(mesh):
    placed = P(None, "shard", "model")
    return jax.shard_map(
        local, mesh=mesh, in_specs=(placed,) * 3, out_specs=(placed, placed), check_vma=False
    )
```

```python
import contextlib

import jax
import jax.numpy as jnp
from jax import lax
from jax.experimental import pallas as pl
from jax.experimental.pallas import tpu as pltpu
from jax.sharding import PartitionSpec as P

MESH = pl.DeviceIdType.MESH
F32 = jnp.float32
ITERS = 4
LINEAR = 3.4445
ROUNDS = 2
PER = 4
BLOCKS = (16, 2, ROUNDS, 64, 128)
hold_rate = 0.9
learn_rate = 0.8
HI = lax.Precision.HIGHEST


def scope(name):
    return contextlib.nullcontext()


def dot(a, b):
    return lax.dot_general(a, b, (((1,), (0,)), ((), ())), precision=HI, preferred_element_type=F32)


def dot_t(a, b):
    return lax.dot_general(a, b, (((1,), (1,)), ((), ())), precision=HI, preferred_element_type=F32)


def merge_halves(a, b):
    low = lax.broadcasted_iota(jnp.int32, a.shape, 1) < 4
    return (
        jnp.where(low, a, pltpu.roll(b, 4, 1)),
        jnp.where(low, pltpu.roll(a, 4, 1), b),
    )


def remote(src, dst, send, recv, to):
    return pltpu.make_async_remote_copy(
        src_ref=src, dst_ref=dst, send_sem=send, recv_sem=recv, device_id=to, device_id_type=MESH
    )


def wait_bytes(ref, sem):
    pltpu.make_async_copy(ref, ref, sem).wait()


def kernel(
    g_hbm, m_hbm, w_hbm, back, moved, held_w,
    gbuf, mbuf, D, R, X, G, GX, S, Z, QR, Y,
    wsem, insem, sent, p1r, xr, zr, qr, p2r, ready,
):
    s, m = lax.axis_index("shard"), lax.axis_index("model")
    zl, yy, core = s // 8, (s // 2) % 4, s % 2
    zh, x = m // 4, m % 4
    side = zl // 2

    loads = []
    for q in range(4):
        c, r = 1 - q % 2, q // 2
        loads.append((
            pltpu.make_async_copy(g_hbm.at[:, c, r], gbuf.at[q], insem.at[q]),
            pltpu.make_async_copy(m_hbm.at[:, c, r], mbuf.at[q], insem.at[q]),
        ))

    def load(q):
        for copy in loads[q]:
            copy.start()

    load(0)

    def group_of(d):
        z = d // 8
        return (zh * (3 - z) + (1 - zh) * z) * 8 + d % 8

    mine = group_of(s)
    partner = ((3 - zl) * 8 + s % 8, (1 - zh) * 4 + x)

    def dest(c, k):
        a, b = k // 4, k % 4
        z = side * a + (1 - side) * (3 - a)
        return z * 8 + ((yy + 2 + b) % 4) * 2 + c

    def late_dest(c, k):
        half, a, b = k // 8, (k % 8) // 2, k % 2
        z = side * a + (1 - side) * (3 - a)
        return z * 8 + (half * 2 + (yy + 1 + b) % 2) * 2 + c

    barrier = pltpu.get_barrier_semaphore()

    @pl.when(zh == 0)
    def _():
        pl.semaphore_signal(barrier, inc=1, device_id=partner, device_id_type=MESH)

    for k in (16, 24, 8):
        for i in range(8):
            pl.semaphore_signal(barrier, inc=1, device_id=((s + k + i) % 32, m), device_id_type=MESH)
    for k in range(1, 8):
        pl.semaphore_signal(barrier, inc=1, device_id=((s + k) % 32, m), device_id_type=MESH)
    for k in range(1, 4):
        pl.semaphore_signal(barrier, inc=1, device_id=(s, zh * 4 + (x + k) % 4), device_id_type=MESH)


    for q in range(4):
        c, r = 1 - q % 2, q // 2
        with scope(f"load#q={q}"):
            for copy in loads[q]:
                copy.wait()
            if q == 0:
                for later in range(1, 4):
                    load(later)

            @pl.loop(0, 8)
            def _(b):
                both = pl.ds(b * 2, 2)
                g = gbuf[q, both]
                D[q, both] = hold_rate * (hold_rate * mbuf[q, both] + g) + g

        if q == 0:
            with scope("barrier"):
                pl.semaphore_wait(barrier, 34 + zh)

            @pl.when(zh == 1)
            def _():
                pl.semaphore_signal(ready, inc=1, device_id=partner, device_id_type=MESH)

        with scope(f"p1send#q={q}"):
            @pl.loop(0, 16)
            def _(k):
                d = dest(c, k)
                rows = D.at[q, group_of(d) // 2]
                place = R.at[r, s // 2, s % 2]

                @pl.when(d != s)
                def _():
                    remote(rows, place, sent, p1r.at[r], (d, m)).start()

                @pl.when(d == s)
                def _():
                    pltpu.make_async_copy(rows, place, p1r.at[r]).start()

    pltpu.make_async_copy(w_hbm, held_w, wsem).start()

    with scope("moved"):
        for q in range(4):
            c, r = 1 - q % 2, q // 2

            @pl.loop(0, 8)
            def _(b):
                both = pl.ds(b * 2, 2)
                moved[both, c, r] = hold_rate * mbuf[q, both] + gbuf[q, both]

    eye = (
        lax.broadcasted_iota(jnp.int32, (128, 128), 0) == lax.broadcasted_iota(jnp.int32, (128, 128), 1)
    ).astype(F32)

    def gram_step(r):
        with scope(f"p1wait#r={r}"):
            wait_bytes(R.at[r], p1r.at[r])

        with scope(f"gram#r={r}"):
            @pl.loop(0, PER)
            def _(j):
                for h in range(2):
                    rows = pl.ds(pl.multiple_of(j * 16 + h * 8, 8), 8)
                    low, high = merge_halves(R[r, :, 0, rows, :], R[r, :, 1, rows, :])
                    X[r, j, :, 256 * h : 256 * h + 128] = low.reshape(128, 128)
                    X[r, j, :, 256 * h + 128 : 256 * h + 256] = high.reshape(128, 128)
                G[r, j] = dot_t(X[r, j], X[r, j])

            for k in range(1, 4):
                q = (x + k) % 4
                remote(G.at[r, q], GX.at[r, 3 - k], sent, xr.at[r], (s, zh * 4 + q)).start()

    def sum_step(r):
        with scope(f"xred#r={r}"):
            wait_bytes(GX.at[r], xr.at[r])
            S[r] = G[r, x] + GX[r, 0] + GX[r, 1] + GX[r, 2]
            if r == 0:
                @pl.when(zh == 0)
                def _():
                    pl.semaphore_wait(ready, 1)

            remote(S.at[r], Z.at[r], sent, zr.at[r], partner).start()

    def chain_step(r):
        with scope(f"zred#r={r}"):
            remote(S.at[r], Z.at[r], sent, zr.at[r], partner).wait_recv()

        with scope(f"chain#r={r}"):
            gram = S[r] + Z[r]
            scale = lax.rsqrt(jnp.sum(jnp.sum(gram * eye, axis=1, keepdims=True), axis=0, keepdims=True) + 1e-06)
            gram = gram * (scale * scale)
            n = []
            for step in range(ITERS):
                n.append(-4.775 * gram + 2.0315 * dot(gram, gram))
                if step < ITERS - 1:
                    mixed = LINEAR * eye + n[-1]
                    gram = dot(dot(mixed, gram), mixed)
            early = LINEAR * (n[0] + n[1]) + dot(n[1], n[0])
            late = LINEAR * (n[2] + n[3]) + dot(n[3], n[2])
            QR[r, x] = (LINEAR**4 * eye + (LINEAR**2 * (early + late) + dot(late, early))) * scale
            for k in range(1, 4):
                to = (s, zh * 4 + (x + k) % 4)
                remote(QR.at[r, x], QR.at[r, x], sent, qr.at[r], to).start()

    def apply_step(r):
        with scope(f"qcast#r={r}"):
            wait_bytes(GX.at[r], qr.at[r])

        with scope(f"apply#r={r}"):
            @pl.loop(0, PER)
            def _(j):
                for h in range(2):
                    wide = dot(QR[r, j], X[r, j, :, 256 * h : 256 * h + 256])
                    rows = pl.ds(pl.multiple_of(j * 16 + h * 8, 8), 8)
                    even, odd = merge_halves(wide[:, :128].reshape(16, 8, 128), wide[:, 128:].reshape(16, 8, 128))
                    Y[r, :, 0, rows, :] = even
                    Y[r, :, 1, rows, :] = odd

        with scope(f"p2send#r={r}"):
            for c in (1, 0):
                @pl.loop(0, 16)
                def _(k):
                    d = late_dest(c, k) if c in (0, 1) else dest(c, k)
                    rows = Y.at[r, d // 2, c]
                    place = back.at[mine // 2, mine % 2, r]

                    @pl.when(d != s)
                    def _():
                        remote(rows, place, sent, p2r.at[r], (d, m)).start()

                    @pl.when(d == s)
                    def _():
                        pltpu.make_async_copy(rows, place, p2r.at[r]).start()

    gram_step(0)
    sum_step(0)
    chain_step(0)

    @pl.when(zh == 1)
    def _():
        gram_step(1)

    apply_step(0)

    @pl.when(jnp.logical_not(zh == 1))
    def _():
        gram_step(1)

    sum_step(1)
    chain_step(1)
    apply_step(1)
    with scope("sendwait"):
        pltpu.make_async_copy(w_hbm, held_w, wsem).wait()
        for ref in (GX, GX, S):
            wait_bytes(ref, sent)
        for _ in range(2):
            wait_bytes(Y.at[:, pl.ds(0, 15)], sent)
            wait_bytes(Y.at[:, 15, 0], sent)

    for r in range(ROUNDS):
        with scope(f"p2wait#r={r}"):
            wait_bytes(R.at[r], p2r.at[r])


def exchange(g, m, w):
    dma = pltpu.SemaphoreType.DMA
    quarters = pltpu.VMEM((4, 16, 64, 128), F32)
    moving = pltpu.VMEM((ROUNDS, 16, 2, 64, 128), F32)
    square = (128, 128)
    return pl.pallas_call(
        kernel,
        out_shape=[jax.ShapeDtypeStruct(BLOCKS, F32)] * 3,
        in_specs=[pl.BlockSpec(memory_space=pltpu.HBM)] * 3,
        out_specs=[pl.BlockSpec(memory_space=pltpu.VMEM)] * 3,
        scratch_shapes=[
            quarters, quarters, quarters,
            moving,
            pltpu.VMEM((ROUNDS, PER, 128, 512), F32),
            pltpu.VMEM((ROUNDS, PER, *square), F32),
            pltpu.VMEM((ROUNDS, 3, *square), F32),
            pltpu.VMEM((ROUNDS, *square), F32),
            pltpu.VMEM((ROUNDS, *square), F32),
            pltpu.VMEM((ROUNDS, PER, *square), F32),
            moving,
            dma(()), dma((4,)), dma(()),
            *[dma((ROUNDS,))] * 5,
            pltpu.SemaphoreType.REGULAR,
        ],
        compiler_params=pltpu.CompilerParams(
            collective_id=0, has_side_effects=True, vmem_limit_bytes=40 * 1024 * 1024
        ),
        name="exchange",
    )(g, m, w)


def finish_kernel(w, back, moved, new_w, new_m, held, wsem, msem):
    momentum_out = pltpu.make_async_copy(moved, new_m, msem)
    momentum_out.start()
    pieces = 8
    size = w.shape[0] // pieces
    for i in range(pieces):
        part = pl.ds(i * size, size)

        @pl.loop(0, size // 128)
        def _(b):
            rows = pl.ds(pl.multiple_of(i * size + b * 128, 128), 128)
            held[rows, :] = w[rows, :] - learn_rate * back[rows, :]

        pltpu.make_async_copy(held.at[part], new_w.at[part], wsem).start()
    pltpu.make_async_copy(held, new_w, wsem).wait()
    momentum_out.wait()


def finish(w, back, moved):
    return pl.pallas_call(
        finish_kernel,
        out_shape=[jax.ShapeDtypeStruct(w.shape, F32)] * 2,
        in_specs=[pl.BlockSpec(memory_space=pltpu.VMEM)] * 3,
        out_specs=[pl.BlockSpec(memory_space=pltpu.HBM)] * 2,
        scratch_shapes=[
            pltpu.VMEM(w.shape, F32),
            pltpu.SemaphoreType.DMA(()),
            pltpu.SemaphoreType.DMA(()),
        ],
        compiler_params=pltpu.CompilerParams(vmem_limit_bytes=16 * 1024 * 1024),
        name="finish",
    )(w, back, moved)


def flat(a):
    return a.reshape(256, 4, 4, 128).transpose(0, 2, 1, 3).reshape(4096, 128)


def unflat(a):
    return a.reshape(256, 4, 4, 128).transpose(0, 2, 1, 3).reshape(256, 4, 512)


def local(gradients, momentum, weights):
    g, m, w = flat(gradients), flat(momentum), flat(weights)
    inputs = [pltpu.with_memory_space_constraint(a.reshape(BLOCKS), pltpu.HBM) for a in (g, m, w)]
    back, moved, w = (a.reshape(4096, 128) for a in exchange(*inputs))
    new_weights, new_momentum = finish(w, back, moved)
    return (unflat(new_weights), unflat(new_momentum))


def solution(mesh):
    placed = P(None, "shard", "model")
    return jax.shard_map(
        local, mesh=mesh, in_specs=(placed,) * 3, out_specs=(placed, placed), check_vma=False
    )
```

```python
import contextlib

import jax
import jax.numpy as jnp
from jax import lax
from jax.experimental import pallas as pl
from jax.experimental.pallas import tpu as pltpu
from jax.sharding import PartitionSpec as P

MESH = pl.DeviceIdType.MESH
F32 = jnp.float32
ITERS = 4
LINEAR = 3.4445
ROUNDS = 2
PER = 4
BLOCKS = (16, 2, ROUNDS, 64, 128)
hold_rate = 0.9
learn_rate = 0.8
HI = lax.Precision.HIGHEST


def scope(name):
    return contextlib.nullcontext()


def dot(a, b):
    return lax.dot_general(a, b, (((1,), (0,)), ((), ())), precision=HI, preferred_element_type=F32)


def dot_t(a, b):
    return lax.dot_general(a, b, (((1,), (1,)), ((), ())), precision=HI, preferred_element_type=F32)


def merge_halves(a, b):
    low = lax.broadcasted_iota(jnp.int32, a.shape, 1) < 4
    return (
        jnp.where(low, a, pltpu.roll(b, 4, 1)),
        jnp.where(low, pltpu.roll(a, 4, 1), b),
    )


def remote(src, dst, send, recv, to):
    return pltpu.make_async_remote_copy(
        src_ref=src, dst_ref=dst, send_sem=send, recv_sem=recv, device_id=to, device_id_type=MESH
    )


def wait_bytes(ref, sem):
    pltpu.make_async_copy(ref, ref, sem).wait()


def kernel(
    g_hbm, m_hbm, w_hbm, back, moved, held_w,
    gbuf, mbuf, D, R, X, G, GX, S, Z, QR, Y,
    wsem, insem, sent, p1r, xr, zr, qr, p2r, ready, ready_x,
):
    s, m = lax.axis_index("shard"), lax.axis_index("model")
    zl, yy, core = s // 8, (s // 2) % 4, s % 2
    zh, x = m // 4, m % 4
    side = zl // 2

    loads = []
    for q in range(4):
        c, r = 1 - q % 2, q // 2
        loads.append((
            pltpu.make_async_copy(g_hbm.at[:, c, r], gbuf.at[q], insem.at[q]),
            pltpu.make_async_copy(m_hbm.at[:, c, r], mbuf.at[q], insem.at[q]),
        ))

    def load(q):
        for copy in loads[q]:
            copy.start()

    load(0)

    def group_of(d):
        z = d // 8
        return (zh * (3 - z) + (1 - zh) * z) * 8 + d % 8

    mine = group_of(s)
    partner = ((3 - zl) * 8 + s % 8, (1 - zh) * 4 + x)

    def dest(c, k):
        a, b = k // 4, k % 4
        z = side * a + (1 - side) * (3 - a)
        return z * 8 + ((yy + 2 + b) % 4) * 2 + c

    def late_dest(c, k):
        a, half, b = k // 4, (k % 4) // 2, k % 2
        z = side * a + (1 - side) * (3 - a)
        return z * 8 + ((yy // 2 + 1 + half) % 2 * 2 + (yy + 1 + b) % 2) * 2 + c

    barrier = pltpu.get_barrier_semaphore()

    @pl.when(zh == 0)
    def _():
        pl.semaphore_signal(barrier, inc=1, device_id=partner, device_id_type=MESH)

    for k in (16, 24, 8):
        for i in range(8):
            pl.semaphore_signal(barrier, inc=1, device_id=((s + k + i) % 32, m), device_id_type=MESH)
    for k in range(1, 8):
        pl.semaphore_signal(barrier, inc=1, device_id=((s + k) % 32, m), device_id_type=MESH)
    for q in range(1, 4):
        @pl.when(x < q)
        def _():
            pl.semaphore_signal(barrier, inc=1, device_id=(s, zh * 4 + q), device_id_type=MESH)


    for q in range(4):
        c, r = 1 - q % 2, q // 2
        with scope(f"load#q={q}"):
            for copy in loads[q]:
                copy.wait()
            if q == 0:
                for later in range(1, 4):
                    load(later)

            @pl.loop(0, 8)
            def _(b):
                both = pl.ds(b * 2, 2)
                g = gbuf[q, both]
                D[q, both] = hold_rate * (hold_rate * mbuf[q, both] + g) + g

        if q == 0:
            with scope("barrier"):
                pl.semaphore_wait(barrier, 31 + x + zh)

            for lower in range(3):
                @pl.when(lower < x)
                def _():
                    pl.semaphore_signal(ready_x, inc=1, device_id=(s, zh * 4 + lower), device_id_type=MESH)

            @pl.when(zh == 1)
            def _():
                pl.semaphore_signal(ready, inc=1, device_id=partner, device_id_type=MESH)

        with scope(f"p1send#q={q}"):
            @pl.loop(0, 16)
            def _(k):
                d = dest(c, k)
                rows = D.at[q, group_of(d) // 2]
                place = R.at[r, s // 2, s % 2]

                @pl.when(d != s)
                def _():
                    remote(rows, place, sent, p1r.at[r], (d, m)).start()

                @pl.when(d == s)
                def _():
                    pltpu.make_async_copy(rows, place, p1r.at[r]).start()

    pltpu.make_async_copy(w_hbm, held_w, wsem).start()

    with scope("moved"):
        for q in range(4):
            c, r = 1 - q % 2, q // 2

            @pl.loop(0, 8)
            def _(b):
                both = pl.ds(b * 2, 2)
                moved[both, c, r] = hold_rate * mbuf[q, both] + gbuf[q, both]

    eye = (
        lax.broadcasted_iota(jnp.int32, (128, 128), 0) == lax.broadcasted_iota(jnp.int32, (128, 128), 1)
    ).astype(F32)

    def gram_step(r):
        with scope(f"p1wait#r={r}"):
            wait_bytes(R.at[r], p1r.at[r])

        with scope(f"gram#r={r}"):
            @pl.loop(0, PER)
            def _(j):
                for h in range(2):
                    rows = pl.ds(pl.multiple_of(j * 16 + h * 8, 8), 8)
                    low, high = merge_halves(R[r, :, 0, rows, :], R[r, :, 1, rows, :])
                    X[r, j, :, 256 * h : 256 * h + 128] = low.reshape(128, 128)
                    X[r, j, :, 256 * h + 128 : 256 * h + 256] = high.reshape(128, 128)
                G[r, j] = dot_t(X[r, j], X[r, j])

            if r == 0:
                @pl.when(x < 3)
                def _():
                    pl.semaphore_wait(ready_x, 3 - x)

            for k in range(1, 4):
                q = (x + k) % 4
                remote(G.at[r, q], GX.at[r, 3 - k], sent, xr.at[r], (s, zh * 4 + q)).start()

    def sum_step(r):
        with scope(f"xred#r={r}"):
            wait_bytes(GX.at[r], xr.at[r])
            S[r] = G[r, x] + GX[r, 0] + GX[r, 1] + GX[r, 2]
            if r == 0:
                @pl.when(zh == 0)
                def _():
                    pl.semaphore_wait(ready, 1)

            remote(S.at[r], Z.at[r], sent, zr.at[r], partner).start()

    def chain_step(r):
        with scope(f"zred#r={r}"):
            remote(S.at[r], Z.at[r], sent, zr.at[r], partner).wait_recv()

        with scope(f"chain#r={r}"):
            gram = S[r] + Z[r]
            scale = lax.rsqrt(jnp.sum(jnp.sum(gram * eye, axis=1, keepdims=True), axis=0, keepdims=True) + 1e-06)
            gram = gram * (scale * scale)
            n = []
            for step in range(ITERS):
                n.append(-4.775 * gram + 2.0315 * dot(gram, gram))
                if step < ITERS - 1:
                    mixed = LINEAR * eye + n[-1]
                    gram = dot(dot(mixed, gram), mixed)
            early = LINEAR * (n[0] + n[1]) + dot(n[1], n[0])
            late = LINEAR * (n[2] + n[3]) + dot(n[3], n[2])
            QR[r, x] = (LINEAR**4 * eye + (LINEAR**2 * (early + late) + dot(late, early))) * scale
            for k in range(1, 4):
                to = (s, zh * 4 + (x + k) % 4)
                remote(QR.at[r, x], QR.at[r, x], sent, qr.at[r], to).start()

    def apply_step(r):
        with scope(f"qcast#r={r}"):
            wait_bytes(GX.at[r], qr.at[r])

        with scope(f"apply#r={r}"):
            @pl.loop(0, PER)
            def _(j):
                for h in range(2):
                    wide = dot(QR[r, j], X[r, j, :, 256 * h : 256 * h + 256])
                    rows = pl.ds(pl.multiple_of(j * 16 + h * 8, 8), 8)
                    even, odd = merge_halves(wide[:, :128].reshape(16, 8, 128), wide[:, 128:].reshape(16, 8, 128))
                    Y[r, :, 0, rows, :] = even
                    Y[r, :, 1, rows, :] = odd

        with scope(f"p2send#r={r}"):
            for c in (1, 0):
                @pl.loop(0, 16)
                def _(k):
                    d = late_dest(c, k) if c in (0, 1) else dest(c, k)
                    rows = Y.at[r, d // 2, c]
                    place = back.at[mine // 2, mine % 2, r]

                    @pl.when(d != s)
                    def _():
                        remote(rows, place, sent, p2r.at[r], (d, m)).start()

                    @pl.when(d == s)
                    def _():
                        pltpu.make_async_copy(rows, place, p2r.at[r]).start()

    gram_step(0)
    sum_step(0)
    chain_step(0)

    @pl.when(zh == 1)
    def _():
        gram_step(1)

    apply_step(0)

    @pl.when(jnp.logical_not(zh == 1))
    def _():
        gram_step(1)

    sum_step(1)
    chain_step(1)
    apply_step(1)
    with scope("sendwait"):
        pltpu.make_async_copy(w_hbm, held_w, wsem).wait()
        for ref in (GX, GX, S):
            wait_bytes(ref, sent)
        for _ in range(2):
            wait_bytes(Y.at[:, pl.ds(0, 15)], sent)
            wait_bytes(Y.at[:, 15, 0], sent)

    for r in range(ROUNDS):
        with scope(f"p2wait#r={r}"):
            wait_bytes(R.at[r], p2r.at[r])


def exchange(g, m, w):
    dma = pltpu.SemaphoreType.DMA
    quarters = pltpu.VMEM((4, 16, 64, 128), F32)
    moving = pltpu.VMEM((ROUNDS, 16, 2, 64, 128), F32)
    square = (128, 128)
    return pl.pallas_call(
        kernel,
        out_shape=[jax.ShapeDtypeStruct(BLOCKS, F32)] * 3,
        in_specs=[pl.BlockSpec(memory_space=pltpu.HBM)] * 3,
        out_specs=[pl.BlockSpec(memory_space=pltpu.VMEM)] * 3,
        scratch_shapes=[
            quarters, quarters, quarters,
            moving,
            pltpu.VMEM((ROUNDS, PER, 128, 512), F32),
            pltpu.VMEM((ROUNDS, PER, *square), F32),
            pltpu.VMEM((ROUNDS, 3, *square), F32),
            pltpu.VMEM((ROUNDS, *square), F32),
            pltpu.VMEM((ROUNDS, *square), F32),
            pltpu.VMEM((ROUNDS, PER, *square), F32),
            moving,
            dma(()), dma((4,)), dma(()),
            *[dma((ROUNDS,))] * 5,
            pltpu.SemaphoreType.REGULAR, pltpu.SemaphoreType.REGULAR,
        ],
        compiler_params=pltpu.CompilerParams(
            collective_id=0, has_side_effects=True, vmem_limit_bytes=40 * 1024 * 1024
        ),
        name="exchange",
    )(g, m, w)


def finish_kernel(w, back, moved, new_w, new_m, held, wsem, msem):
    momentum_out = pltpu.make_async_copy(moved, new_m, msem)
    momentum_out.start()
    pieces = 8
    size = w.shape[0] // pieces
    for i in range(pieces):
        part = pl.ds(i * size, size)

        @pl.loop(0, size // 128)
        def _(b):
            rows = pl.ds(pl.multiple_of(i * size + b * 128, 128), 128)
            held[rows, :] = w[rows, :] - learn_rate * back[rows, :]

        pltpu.make_async_copy(held.at[part], new_w.at[part], wsem).start()
    pltpu.make_async_copy(held, new_w, wsem).wait()
    momentum_out.wait()


def finish(w, back, moved):
    return pl.pallas_call(
        finish_kernel,
        out_shape=[jax.ShapeDtypeStruct(w.shape, F32)] * 2,
        in_specs=[pl.BlockSpec(memory_space=pltpu.VMEM)] * 3,
        out_specs=[pl.BlockSpec(memory_space=pltpu.HBM)] * 2,
        scratch_shapes=[
            pltpu.VMEM(w.shape, F32),
            pltpu.SemaphoreType.DMA(()),
            pltpu.SemaphoreType.DMA(()),
        ],
        compiler_params=pltpu.CompilerParams(vmem_limit_bytes=16 * 1024 * 1024),
        name="finish",
    )(w, back, moved)


def flat(a):
    return a.reshape(256, 4, 4, 128).transpose(0, 2, 1, 3).reshape(4096, 128)


def unflat(a):
    return a.reshape(256, 4, 4, 128).transpose(0, 2, 1, 3).reshape(256, 4, 512)


def local(gradients, momentum, weights):
    g, m, w = flat(gradients), flat(momentum), flat(weights)
    inputs = [pltpu.with_memory_space_constraint(a.reshape(BLOCKS), pltpu.HBM) for a in (g, m, w)]
    back, moved, w = (a.reshape(4096, 128) for a in exchange(*inputs))
    new_weights, new_momentum = finish(w, back, moved)
    return (unflat(new_weights), unflat(new_momentum))


def solution(mesh):
    placed = P(None, "shard", "model")
    return jax.shard_map(
        local, mesh=mesh, in_specs=(placed,) * 3, out_specs=(placed, placed), check_vma=False
    )
```

```python
import contextlib

import jax
import jax.numpy as jnp
from jax import lax
from jax.experimental import pallas as pl
from jax.experimental.pallas import tpu as pltpu
from jax.sharding import PartitionSpec as P

MESH = pl.DeviceIdType.MESH
F32 = jnp.float32
ITERS = 4
LINEAR = 3.4445
ROUNDS = 2
PER = 4
BLOCKS = (16, 2, ROUNDS, 64, 128)
hold_rate = 0.9
learn_rate = 0.8
HI = lax.Precision.HIGHEST


def scope(name):
    return contextlib.nullcontext()


def dot(a, b):
    return lax.dot_general(a, b, (((1,), (0,)), ((), ())), precision=HI, preferred_element_type=F32)


def dot_t(a, b):
    return lax.dot_general(a, b, (((1,), (1,)), ((), ())), precision=HI, preferred_element_type=F32)


def merge_halves(a, b):
    low = lax.broadcasted_iota(jnp.int32, a.shape, 1) < 4
    return (
        jnp.where(low, a, pltpu.roll(b, 4, 1)),
        jnp.where(low, pltpu.roll(a, 4, 1), b),
    )


def remote(src, dst, send, recv, to):
    return pltpu.make_async_remote_copy(
        src_ref=src, dst_ref=dst, send_sem=send, recv_sem=recv, device_id=to, device_id_type=MESH
    )


def wait_bytes(ref, sem):
    pltpu.make_async_copy(ref, ref, sem).wait()


def kernel(
    g_hbm, m_hbm, w_hbm, back, moved, held_w,
    gbuf, mbuf, D, R, X, G, GX, S, Z, QR, Y,
    wsem, insem, sent, p1r, xr, zr, qr, p2r, ready, ready_x,
):
    s, m = lax.axis_index("shard"), lax.axis_index("model")
    zl, yy, core = s // 8, (s // 2) % 4, s % 2
    zh, x = m // 4, m % 4
    side = zl // 2

    loads = []
    for q in range(4):
        c, r = 1 - q % 2, q // 2
        loads.append((
            pltpu.make_async_copy(g_hbm.at[:, c, r], gbuf.at[q], insem.at[q]),
            pltpu.make_async_copy(m_hbm.at[:, c, r], mbuf.at[q], insem.at[q]),
        ))

    def load(q):
        for copy in loads[q]:
            copy.start()

    load(0)

    def group_of(d):
        z = d // 8
        return (zh * (3 - z) + (1 - zh) * z) * 8 + d % 8

    mine = group_of(s)
    partner = ((3 - zl) * 8 + s % 8, (1 - zh) * 4 + x)

    def dest(c, k):
        a, b = k // 4, k % 4
        z = side * a + (1 - side) * (3 - a)
        return z * 8 + ((yy + 2 + b) % 4) * 2 + c

    def late_dest(c, k):
        half, a, b = k // 8, (k % 8) // 2, k % 2
        z = side * a + (1 - side) * (3 - a)
        return z * 8 + (half * 2 + (yy + 1 + b) % 2) * 2 + c

    barrier = pltpu.get_barrier_semaphore()

    @pl.when(zh == 0)
    def _():
        pl.semaphore_signal(barrier, inc=1, device_id=partner, device_id_type=MESH)

    for k in (16, 24, 8):
        for i in range(8):
            pl.semaphore_signal(barrier, inc=1, device_id=((s + k + i) % 32, m), device_id_type=MESH)
    for k in range(1, 8):
        pl.semaphore_signal(barrier, inc=1, device_id=((s + k) % 32, m), device_id_type=MESH)
    for q in range(1, 4):
        @pl.when(x < q)
        def _():
            pl.semaphore_signal(barrier, inc=1, device_id=(s, zh * 4 + q), device_id_type=MESH)


    for q in range(4):
        c, r = 1 - q % 2, q // 2
        with scope(f"load#q={q}"):
            for copy in loads[q]:
                copy.wait()
            if q == 0:
                for later in range(1, 4):
                    load(later)

            @pl.loop(0, 8)
            def _(b):
                both = pl.ds(b * 2, 2)
                g = gbuf[q, both]
                D[q, both] = hold_rate * (hold_rate * mbuf[q, both] + g) + g

        if q == 0:
            with scope("barrier"):
                pl.semaphore_wait(barrier, 31 + x + zh)

            for lower in range(3):
                @pl.when(lower < x)
                def _():
                    pl.semaphore_signal(ready_x, inc=1, device_id=(s, zh * 4 + lower), device_id_type=MESH)

            @pl.when(zh == 1)
            def _():
                pl.semaphore_signal(ready, inc=1, device_id=partner, device_id_type=MESH)

        with scope(f"p1send#q={q}"):
            @pl.loop(0, 16)
            def _(k):
                d = dest(c, k)
                rows = D.at[q, group_of(d) // 2]
                place = R.at[r, s // 2, s % 2]

                @pl.when(d != s)
                def _():
                    remote(rows, place, sent, p1r.at[r], (d, m)).start()

                @pl.when(d == s)
                def _():
                    pltpu.make_async_copy(rows, place, p1r.at[r]).start()

    pltpu.make_async_copy(w_hbm, held_w, wsem).start()

    with scope("moved"):
        for q in range(4):
            c, r = 1 - q % 2, q // 2

            @pl.loop(0, 8)
            def _(b):
                both = pl.ds(b * 2, 2)
                moved[both, c, r] = hold_rate * mbuf[q, both] + gbuf[q, both]

    eye = (
        lax.broadcasted_iota(jnp.int32, (128, 128), 0) == lax.broadcasted_iota(jnp.int32, (128, 128), 1)
    ).astype(F32)

    def gram_step(r):
        with scope(f"p1wait#r={r}"):
            wait_bytes(R.at[r], p1r.at[r])

        with scope(f"gram#r={r}"):
            @pl.loop(0, PER)
            def _(j):
                for h in range(2):
                    rows = pl.ds(pl.multiple_of(j * 16 + h * 8, 8), 8)
                    low, high = merge_halves(R[r, :, 0, rows, :], R[r, :, 1, rows, :])
                    X[r, j, :, 256 * h : 256 * h + 128] = low.reshape(128, 128)
                    X[r, j, :, 256 * h + 128 : 256 * h + 256] = high.reshape(128, 128)
                G[r, j] = dot_t(X[r, j], X[r, j])

            if r == 0:
                @pl.when(x < 3)
                def _():
                    pl.semaphore_wait(ready_x, 3 - x)

            for k in range(1, 4):
                q = (x + k) % 4
                remote(G.at[r, q], GX.at[r, 3 - k], sent, xr.at[r], (s, zh * 4 + q)).start()

    def sum_step(r):
        with scope(f"xred#r={r}"):
            wait_bytes(GX.at[r], xr.at[r])
            S[r] = G[r, x] + GX[r, 0] + GX[r, 1] + GX[r, 2]
            if r == 0:
                @pl.when(zh == 0)
                def _():
                    pl.semaphore_wait(ready, 1)

            remote(S.at[r], Z.at[r], sent, zr.at[r], partner).start()

    def chain_step(r):
        with scope(f"zred#r={r}"):
            remote(S.at[r], Z.at[r], sent, zr.at[r], partner).wait_recv()

        with scope(f"chain#r={r}"):
            gram = S[r] + Z[r]
            scale = lax.rsqrt(jnp.sum(jnp.sum(gram * eye, axis=1, keepdims=True), axis=0, keepdims=True) + 1e-06)
            gram = gram * (scale * scale)
            n = []
            for step in range(ITERS):
                n.append(-4.775 * gram + 2.0315 * dot(gram, gram))
                if step < ITERS - 1:
                    mixed = LINEAR * eye + n[-1]
                    gram = dot(dot(mixed, gram), mixed)
            early = LINEAR * (n[0] + n[1]) + dot(n[1], n[0])
            late = LINEAR * (n[2] + n[3]) + dot(n[3], n[2])
            QR[r, x] = (LINEAR**4 * eye + (LINEAR**2 * (early + late) + dot(late, early))) * scale
            for k in range(1, 4):
                to = (s, zh * 4 + (x + k) % 4)
                remote(QR.at[r, x], QR.at[r, x], sent, qr.at[r], to).start()

    def apply_step(r):
        with scope(f"qcast#r={r}"):
            wait_bytes(GX.at[r], qr.at[r])

        with scope(f"apply#r={r}"):
            @pl.loop(0, PER)
            def _(j):
                for h in range(2):
                    wide = dot(QR[r, j], X[r, j, :, 256 * h : 256 * h + 256])
                    rows = pl.ds(pl.multiple_of(j * 16 + h * 8, 8), 8)
                    even, odd = merge_halves(wide[:, :128].reshape(16, 8, 128), wide[:, 128:].reshape(16, 8, 128))
                    Y[r, :, 0, rows, :] = even
                    Y[r, :, 1, rows, :] = odd

        with scope(f"p2send#r={r}"):
            for c in (1, 0):
                @pl.loop(0, 16)
                def _(k):
                    d = late_dest(c, k) if c in (0, 1) else dest(c, k)
                    rows = Y.at[r, d // 2, c]
                    place = back.at[mine // 2, mine % 2, r]

                    @pl.when(d != s)
                    def _():
                        remote(rows, place, sent, p2r.at[r], (d, m)).start()

                    @pl.when(d == s)
                    def _():
                        pltpu.make_async_copy(rows, place, p2r.at[r]).start()

    gram_step(0)
    sum_step(0)
    chain_step(0)

    @pl.when(zh == 1)
    def _():
        gram_step(1)

    apply_step(0)

    @pl.when(jnp.logical_not(zh == 1))
    def _():
        gram_step(1)

    sum_step(1)
    chain_step(1)
    apply_step(1)
    with scope("sendwait"):
        pltpu.make_async_copy(w_hbm, held_w, wsem).wait()
        for ref in (GX, GX, S):
            wait_bytes(ref, sent)
        for _ in range(2):
            wait_bytes(Y.at[:, pl.ds(0, 15)], sent)
            wait_bytes(Y.at[:, 15, 0], sent)

    for r in range(ROUNDS):
        with scope(f"p2wait#r={r}"):
            wait_bytes(R.at[r], p2r.at[r])


def exchange(g, m, w):
    dma = pltpu.SemaphoreType.DMA
    quarters = pltpu.VMEM((4, 16, 64, 128), F32)
    moving = pltpu.VMEM((ROUNDS, 16, 2, 64, 128), F32)
    square = (128, 128)
    return pl.pallas_call(
        kernel,
        out_shape=[jax.ShapeDtypeStruct(BLOCKS, F32)] * 3,
        in_specs=[pl.BlockSpec(memory_space=pltpu.HBM)] * 3,
        out_specs=[pl.BlockSpec(memory_space=pltpu.VMEM)] * 3,
        scratch_shapes=[
            quarters, quarters, quarters,
            moving,
            pltpu.VMEM((ROUNDS, PER, 128, 512), F32),
            pltpu.VMEM((ROUNDS, PER, *square), F32),
            pltpu.VMEM((ROUNDS, 3, *square), F32),
            pltpu.VMEM((ROUNDS, *square), F32),
            pltpu.VMEM((ROUNDS, *square), F32),
            pltpu.VMEM((ROUNDS, PER, *square), F32),
            moving,
            dma(()), dma((4,)), dma(()),
            *[dma((ROUNDS,))] * 5,
            pltpu.SemaphoreType.REGULAR, pltpu.SemaphoreType.REGULAR,
        ],
        compiler_params=pltpu.CompilerParams(
            collective_id=0, has_side_effects=True, vmem_limit_bytes=40 * 1024 * 1024
        ),
        name="exchange",
    )(g, m, w)


def finish_kernel(w, back, moved, new_w, new_m, held, wsem, msem):
    momentum_out = pltpu.make_async_copy(moved, new_m, msem)
    momentum_out.start()
    pieces = 8
    size = w.shape[0] // pieces
    for i in range(pieces):
        part = pl.ds(i * size, size)

        @pl.loop(0, size // 128)
        def _(b):
            rows = pl.ds(pl.multiple_of(i * size + b * 128, 128), 128)
            held[rows, :] = w[rows, :] - learn_rate * back[rows, :]

        pltpu.make_async_copy(held.at[part], new_w.at[part], wsem).start()
    pltpu.make_async_copy(held, new_w, wsem).wait()
    momentum_out.wait()


def finish(w, back, moved):
    return pl.pallas_call(
        finish_kernel,
        out_shape=[jax.ShapeDtypeStruct(w.shape, F32)] * 2,
        in_specs=[pl.BlockSpec(memory_space=pltpu.VMEM)] * 3,
        out_specs=[pl.BlockSpec(memory_space=pltpu.HBM)] * 2,
        scratch_shapes=[
            pltpu.VMEM(w.shape, F32),
            pltpu.SemaphoreType.DMA(()),
            pltpu.SemaphoreType.DMA(()),
        ],
        compiler_params=pltpu.CompilerParams(vmem_limit_bytes=16 * 1024 * 1024),
        name="finish",
    )(w, back, moved)


def flat(a):
    return a.reshape(256, 4, 4, 128).transpose(0, 2, 1, 3).reshape(4096, 128)


def unflat(a):
    return a.reshape(256, 4, 4, 128).transpose(0, 2, 1, 3).reshape(256, 4, 512)


def local(gradients, momentum, weights):
    g, m, w = flat(gradients), flat(momentum), flat(weights)
    inputs = [pltpu.with_memory_space_constraint(a.reshape(BLOCKS), pltpu.HBM) for a in (g, m, w)]
    back, moved, w = (a.reshape(4096, 128) for a in exchange(*inputs))
    new_weights, new_momentum = finish(w, back, moved)
    return (unflat(new_weights), unflat(new_momentum))


def solution(mesh):
    placed = P(None, "shard", "model")
    return jax.shard_map(
        local, mesh=mesh, in_specs=(placed,) * 3, out_specs=(placed, placed), check_vma=False
    )
```
